32 devices in a mesh: seq: 16 (over z, y, core), fsdp: 2 (over x).
Axes of the slice: x: 2, y: 2, z: 4, core: 2. Of those that a mesh axis runs over, the one named last changes fastest.
Arguments:
- residual: bfloat16 [2, 1024, 1440], P('fsdp', 'seq'), may hold values from -40 to 40
- queries: bfloat16 [2, 1024, 2048], P('fsdp', 'seq'), may hold values from -64 to 64
- key_rows: bfloat16 [2, 1024, 256], P('fsdp', 'seq'), may hold values from -16 to 16
- values: bfloat16 [2, 1024, 256], P('fsdp', 'seq'), may hold values from -1 to 2
- attention_sinks: float32 [32], replicated, may hold values from 0 to 6
- out_weight: bfloat16 [2048, 1440], P('seq', 'fsdp'), may hold values from -0.125 to 0.125
- norm_gain: bfloat16 [1440], replicated, may hold values from 0.25 to 1.75
- router_weight: bfloat16 [1440, 16], replicated, may hold values from -0.15625 to 0.15625
- gate_weight: bfloat16 [1440, 23040], P(None, 'seq'), may hold values from -0.15625 to 0.15625
- up_weight: bfloat16 [1440, 23040], P(None, 'seq'), may hold values from -0.15625 to 0.15625
- down_weight: bfloat16 [23040, 1440], P('seq'), may hold values from -0.15625 to 0.15625
- routing: int32 [2, 1024, 2], P('fsdp', 'seq'), may hold values from 0 to 15, as said below
- span_order: int32 [32], replicated, may hold values from 0 to 31, as said below
Outputs:
- attended: bfloat16 [2, 1024, 1440], P('fsdp', 'seq')
- layer_output: bfloat16 [2, 1024, 1440], P('fsdp', 'seq')
The draws below stay inside these ranges and needn't reach their ends.
Inputs may be any that keep to these rules, and one draw needn't show every extreme that they name: A permutation of 0 to 31; index i of seq holds the rows of spans span_order[2 i] and span_order[2 i + 1], and these two add up to 31. `routing`: in the rows of one device no expert is named more than 12 times; in each prompt one expert is named exactly 12 times in the rows of every device; the 2 experts of a row differ.
All inputs are finite; a program needn't handle non-finite values.
Results may differ from the reference program's by a relative error of at most 0.009.
Values may be sent and summed in bfloat16 or wider, within the bound.
A program may use at most 64 MiB of HBM per device.

```python
import jax
import jax.numpy as jnp
from jax import lax

D = 1440
HEADS = 32
KVH = 4
HD = 64
EXPERTS = 16
FFE = 1440
TOPK = 2
TOK_DEV = 64
HALF = 32
CAP = 12
PROMPTS = 2
TOKENS = 1024
SPANS = 32
UNITS = 1440
N_SEQ = 16


def draw_residual(key, part):
    noise_part = jax.random.normal(jax.random.fold_in(key, 7), (PROMPTS, TOKENS, D), jnp.float32)
    return jnp.clip(noise_part, -40.0, 40.0).astype(jnp.bfloat16)


def draw_queries(key, part):
    noise_key = jax.random.fold_in(key, 3)
    drawn = jax.random.normal(noise_key, (PROMPTS, TOKENS, HEADS, HD), jnp.float32)
    return jnp.clip(drawn, -64.0, 64.0).reshape(PROMPTS, TOKENS, HEADS * HD).astype(jnp.bfloat16)


def draw_key_rows(key, part):
    noise_key = jax.random.fold_in(key, 5)
    drawn = jax.random.normal(noise_key, (PROMPTS, TOKENS, KVH, HD), jnp.float32)
    return jnp.clip(drawn, -16.0, 16.0).reshape(PROMPTS, TOKENS, KVH * HD).astype(jnp.bfloat16)


def draw_span_order(key, part):
    pair_index = jax.random.permutation(jax.random.fold_in(key, 21), SPANS // 2).astype(jnp.int32)
    flip_order = jax.random.randint(jax.random.fold_in(key, 22), (SPANS // 2,), 0, 2).astype(jnp.int32)
    first_span = jnp.where(flip_order == 1, SPANS - 1 - pair_index, pair_index)
    return jnp.stack([first_span, SPANS - 1 - first_span], axis=1).reshape(SPANS).astype(jnp.int32)


def route_block(block_key, hot_expert):
    perm_key, order_key, turn_key = jax.random.split(block_key, 3)
    spare_slots = jax.random.permutation(perm_key, (EXPERTS - 1) * CAP)[:TOK_DEV * TOPK - CAP]
    others = (jnp.sort(spare_slots) // CAP).astype(jnp.int32)
    others = others + (others >= hot_expert).astype(jnp.int32)
    listed = jnp.concatenate([jnp.full((CAP,), hot_expert, jnp.int32), others])
    table_rows = listed.reshape(TOPK, TOK_DEV).T
    table_rows = table_rows[jax.random.permutation(order_key, TOK_DEV)]
    turn_by = jax.random.randint(turn_key, (TOK_DEV, 1), 0, TOPK)
    column_order = (jnp.arange(TOPK, dtype=jnp.int32)[None, :] + turn_by) % TOPK
    return jnp.take_along_axis(table_rows, column_order, axis=1).astype(jnp.int32)


def draw_routing(key, part):
    blocks = TOKENS // TOK_DEV
    hot_experts = jax.random.randint(jax.random.fold_in(key, 31), (PROMPTS,), 0, EXPERTS).astype(jnp.int32)
    block_keys = jax.random.split(jax.random.fold_in(key, 32), PROMPTS * blocks)
    hot_each = jnp.repeat(hot_experts, blocks)
    tables = jax.vmap(route_block)(block_keys, hot_each)
    return tables.reshape(PROMPTS, TOKENS, TOPK).astype(jnp.int32)


def steps_of(own_key, dims, pieces, low, top_value):
    def one(axis_at, shards_of):
        steps = jax.random.uniform(jax.random.fold_in(jax.random.fold_in(own_key, 6), axis_at), (shards_of,), jnp.float32, low / len(pieces), top_value / len(pieces))
        return jnp.repeat(jnp.exp(steps), dims[axis_at] // shards_of).reshape((-1,) + (1,) * (len(dims) - axis_at - 1))

    level = one(*pieces[0])
    for cut in pieces[1:]:
        level = level * one(*cut)
    return level


def gaussian(stream_key, dims, scale, bound, shards=(), kind=jnp.bfloat16):
    values = jax.random.normal(stream_key, dims, jnp.float32) * scale
    if len(shards) > 0:
        values = steps_of(stream_key, dims, shards, -0.22, 0.18) * values
    return jnp.clip(values, min=-bound, max=bound).astype(kind)


def setup_inputs(seed: int = 0) -> dict:
    splits = jax.random.split(jax.random.key(seed), 14)
    residual = draw_residual(jax.random.fold_in(splits[13], 71), 0)
    queries = draw_queries(jax.random.fold_in(splits[13], 71), 0)
    key_rows = draw_key_rows(jax.random.fold_in(splits[13], 71), 0)
    values = jnp.clip(-1.0 + 3.0 * jax.random.uniform(splits[3], (PROMPTS, TOKENS, KVH * HD), jnp.float32) ** steps_of(splits[3], (PROMPTS, TOKENS, KVH * HD), ((0, 2), (1, 16)), -0.2, 0.2), -1.0, 2.0).astype(jnp.bfloat16)
    attention_sinks = jnp.clip(jax.random.uniform(splits[4], (HEADS,), jnp.float32, 0.0, 6.0), 0.0, 6.0)
    out_weight = gaussian(splits[5], (HEADS * HD, D), (HEADS * HD) ** -0.5, 0.125, ((0, 16), (1, 2)))
    norm_gain = jnp.clip(1.0 + 0.15 * jax.random.normal(splits[6], (D,), jnp.float32), 0.25, 1.75).astype(jnp.bfloat16)
    router_weight = gaussian(splits[7], (D, EXPERTS), D ** -0.5, 0.15625)
    gate_weight = gaussian(splits[8], (D, EXPERTS * FFE), D ** -0.5, 0.15625, ((1, 16),))
    up_weight = gaussian(splits[9], (D, EXPERTS * FFE), D ** -0.5, 0.15625, ((1, 16),))
    down_weight = gaussian(splits[10], (EXPERTS * FFE, D), FFE ** -0.5, 0.15625, ((0, 16),))
    routing = draw_routing(jax.random.fold_in(splits[13], 71), 0)
    span_order = draw_span_order(jax.random.fold_in(splits[13], 71), 0)
    return dict(residual=residual, queries=queries, key_rows=key_rows, values=values, attention_sinks=attention_sinks, out_weight=out_weight, norm_gain=norm_gain, router_weight=router_weight, gate_weight=gate_weight, up_weight=up_weight, down_weight=down_weight, routing=routing, span_order=span_order)


rope_base = 150000.0
norm_eps = 1e-05
masked_score = -1e+30

def lookup(table_values, lookup_index):
    matches = lookup_index[:, None] == jnp.arange(table_values.shape[0], dtype=jnp.int32)[None, :]
    return lax.optimization_barrier(jnp.sum(jnp.where(matches, table_values[None, :], 0), axis=1)).astype(jnp.int32)

def positions(span_order, row_index):
    device = row_index // TOK_DEV
    within = row_index % TOK_DEV
    span_index = lookup(span_order, 2 * device + within // HALF)
    return span_index * HALF + within % HALF

def rotate(head_values, where_at):
    half_size = head_values.shape[-1] // 2
    frequency = jnp.exp(-jnp.log(rope_base) * jnp.arange(half_size, dtype=jnp.float32) / half_size)
    angles = where_at.astype(jnp.float32)[:, None] * frequency[None, :]
    cosine = jnp.cos(angles)[:, None, :]
    sine_part = jnp.sin(angles)[:, None, :]
    first_half = head_values[..., :half_size]
    second = head_values[..., half_size:]
    return jnp.concatenate([first_half * cosine - second * sine_part, second * cosine + first_half * sine_part], axis=-1)

def slot_of(chosen):
    flattened = chosen.reshape(-1)
    onehot = (flattened[:, None] == jnp.arange(EXPERTS, dtype=jnp.int32)[None, :]).astype(jnp.int32)
    before = jnp.cumsum(onehot, axis=0) - onehot
    return lax.optimization_barrier(jnp.sum(before * onehot, axis=1)).reshape(chosen.shape).astype(jnp.int32)

def reference(residual, queries, key_rows, values, attention_sinks, out_weight, norm_gain, router_weight, gate_weight, up_weight, down_weight, routing, span_order):
    where_at = positions(span_order, jnp.arange(TOKENS, dtype=jnp.int32))
    visible = where_at[None, :] <= where_at[:, None]
    score_scale = HD ** (-0.5)
    group_size = HEADS // KVH

    def attend_prompt(operands):
        query_prompt, key_prompt, value_prompt = operands
        query_rot = rotate(query_prompt.astype(jnp.float32).reshape(TOKENS, HEADS, HD), where_at).astype(jnp.bfloat16)
        key_rot = rotate(key_prompt.astype(jnp.float32).reshape(TOKENS, KVH, HD), where_at).astype(jnp.bfloat16)
        value_heads = value_prompt.reshape(TOKENS, KVH, HD)

        def attend_head(head_index):
            group_index = head_index // group_size
            query_one = lax.dynamic_index_in_dim(query_rot, head_index, 1, keepdims=False).astype(jnp.float32)
            key_one = lax.dynamic_index_in_dim(key_rot, group_index, 1, keepdims=False).astype(jnp.float32)
            value_one = lax.dynamic_index_in_dim(value_heads, group_index, 1, keepdims=False)
            sink_one = lax.dynamic_index_in_dim(attention_sinks, head_index, 0, keepdims=False).astype(jnp.float32)
            scores = jnp.dot(query_one, key_one.T, preferred_element_type=jnp.float32, precision=lax.Precision.HIGHEST) * score_scale
            scores = jnp.where(visible, scores, masked_score)
            row_max = jnp.maximum(lax.optimization_barrier(jnp.max(scores, axis=1)), sink_one)
            weight = jnp.exp(scores - row_max[:, None])
            denominator = lax.optimization_barrier(jnp.sum(weight, axis=1)) + jnp.exp(sink_one - row_max)
            weighted = jnp.dot(weight.astype(jnp.bfloat16), value_one, preferred_element_type=jnp.float32)
            return weighted / denominator[:, None]
        heads_out = lax.map(attend_head, jnp.arange(HEADS, dtype=jnp.int32))
        return jnp.transpose(heads_out, (1, 0, 2)).reshape(TOKENS, HEADS * HD).astype(jnp.bfloat16)
    attention_rows = lax.map(attend_prompt, (queries, key_rows, values))
    attended = jnp.dot(attention_rows.reshape(PROMPTS * TOKENS, HEADS * HD), out_weight, preferred_element_type=jnp.float32).astype(jnp.bfloat16)
    attended = attended.reshape(PROMPTS, TOKENS, D)
    stream = residual.astype(jnp.float32) + attended.astype(jnp.float32)
    normed = (stream * lax.rsqrt(lax.optimization_barrier(jnp.mean(stream * stream, axis=-1, keepdims=True)) + norm_eps) * norm_gain.astype(jnp.float32)).astype(jnp.bfloat16)
    logits = jnp.dot(normed.reshape(PROMPTS * TOKENS, D), router_weight, preferred_element_type=jnp.float32).reshape(PROMPTS, TOKENS, EXPERTS)
    selected = jnp.take_along_axis(logits, routing, axis=-1)
    gates = 1.0 / lax.optimization_barrier(jnp.sum(jnp.exp(selected[..., :, None] - selected[..., None, :]), axis=-2))

    def expert_prompt(operands):
        normed_prompt, chosen_prompt, gates_prompt = operands
        blocks_in = normed_prompt.reshape(N_SEQ, TOK_DEV, D)
        chosen_blocks = chosen_prompt.reshape(N_SEQ, TOK_DEV, TOPK)
        slot_blocks = jax.vmap(slot_of)(chosen_blocks)
        target = chosen_blocks * CAP + slot_blocks

        def dispatch_one(target_block, rows_block):
            mapping = lax.optimization_barrier(jnp.sum((target_block[None, :, :] == jnp.arange(EXPERTS * CAP, dtype=jnp.int32)[:, None, None]).astype(jnp.int32), axis=2))
            return jnp.dot(mapping.astype(jnp.bfloat16), rows_block, preferred_element_type=jnp.float32).astype(jnp.bfloat16)
        buffers = jax.vmap(dispatch_one)(target, blocks_in).reshape(N_SEQ, EXPERTS, CAP, D)

        def run_one(expert_index):
            expert_rows = lax.dynamic_index_in_dim(buffers, expert_index, 1, keepdims=False).reshape(N_SEQ * CAP, D)
            gate_columns = lax.dynamic_slice_in_dim(gate_weight, (expert_index * FFE).astype(jnp.int32), FFE, 1)
            up_columns = lax.dynamic_slice_in_dim(up_weight, (expert_index * FFE).astype(jnp.int32), FFE, 1)
            down_rows = lax.dynamic_slice_in_dim(down_weight, (expert_index * FFE).astype(jnp.int32), FFE, 0)
            gate_values = jnp.dot(expert_rows, gate_columns, preferred_element_type=jnp.float32)
            up_values = jnp.dot(expert_rows, up_columns, preferred_element_type=jnp.float32)
            hidden = (gate_values * jax.nn.sigmoid(1.702 * gate_values) * (up_values + 1.0)).astype(jnp.bfloat16)
            parts = jnp.einsum('rgu,gud->rgd', hidden.reshape(N_SEQ * CAP, FFE // UNITS, UNITS).astype(jnp.float32), down_rows.reshape(FFE // UNITS, UNITS, D).astype(jnp.float32))
            rounded = lax.optimization_barrier(parts.astype(jnp.bfloat16))
            return lax.optimization_barrier(jnp.sum(rounded.astype(jnp.float32), axis=1))
        outputs = lax.map(run_one, jnp.arange(EXPERTS, dtype=jnp.int32)).reshape(EXPERTS * N_SEQ * CAP, D)
        device_index = jnp.arange(N_SEQ, dtype=jnp.int32)[:, None, None]
        flat_index = ((chosen_blocks * N_SEQ + device_index) * CAP + slot_blocks).reshape(-1).astype(jnp.int32)
        chosen_out = jnp.take(outputs, flat_index, axis=0).reshape(TOKENS, TOPK, D)
        return lax.optimization_barrier(jnp.sum(chosen_out * gates_prompt[:, :, None], axis=1))
    expert_mix = lax.map(expert_prompt, (normed, routing, gates))
    layer_output = (stream + expert_mix).astype(jnp.bfloat16)
    return (attended, layer_output)
```

```python
import functools

import jax
import jax.numpy as jnp
from jax import lax
from jax.experimental import pallas as pl
from jax.experimental.pallas import tpu as pltpu
from jax.sharding import PartitionSpec as P

D = 1440
HEADS = 32
KVH = 4
HD = 64
EXPERTS = 16
TOPK = 2
TOK_DEV = 64
HALF = 32
CAP = 12


rope_base = 150000.0
norm_eps = 1e-05
masked_score = -1e30


MESH = pl.DeviceIdType.MESH


def remote(source, target, send_sem, recv_sem, **where):
    return pltpu.make_async_remote_copy(
        src_ref=source,
        dst_ref=target,
        send_sem=send_sem,
        recv_sem=recv_sem,
        device_id=where,
        device_id_type=MESH,
    )


def greet(peers):
    barrier = pltpu.get_barrier_semaphore()
    for where in peers:
        pl.semaphore_signal(barrier, inc=1, device_id=where, device_id_type=MESH)
    pl.semaphore_wait(barrier, len(peers))


def gather_plan(block, slots, sems, z_count, z, y, c):
    z_send, z_recv, y_send, y_recv, c_send, c_recv, own_sem = sems

    def slot(zz, yy, cc):
        return (zz * 2 + yy) * 2 + cc

    def z_of(d):
        return lax.rem(z + z_count - d, z_count)

    own = slot(z, y, c)
    to_z = [
        remote(block, slots.at[own], z_send.at[d], z_recv.at[d], seq=slot(lax.rem(z + d, z_count), y, c))
        for d in range(1, z_count)
    ]

    def to_y(d):
        source = block if d == 0 else slots.at[slot(z_of(d), y, c)]
        return remote(source, slots.at[slot(z_of(d), y, c)], y_send.at[d], y_recv.at[d], seq=slot(z, 1 - y, c))

    def to_c(side, d):
        index = slot(z_of(d), y if side == 0 else 1 - y, c)
        source = block if side == 0 and d == 0 else slots.at[index]
        return remote(source, slots.at[index], c_send.at[side, d], c_recv.at[side, d], seq=slot(z, y, 1 - c))

    local = pltpu.make_async_copy(block, slots.at[own], own_sem)
    ys = [to_y(d) for d in range(z_count)]
    cs = [[to_c(side, d) for d in range(z_count)] for side in range(2)]

    def start_z():
        local.start()
        for copy in to_z:
            copy.start()

    def relay(d):
        if d > 0:
            to_z[d - 1].wait_recv()
        ys[d].start()
        cs[0][d].start()

    def relay_across(d):
        ys[d].wait_recv()
        cs[1][d].start()

    def finish():
        for side in range(2):
            for d in range(z_count):
                cs[side][d].wait_recv()
        local.wait()

    def drain():
        for copy in to_z + ys + cs[0] + cs[1]:
            copy.wait_send()

    return start_z, relay, relay_across, finish, drain


def layer_kernel(
    seq_count, fsdp_count,
    sink_ref, span_ref, gain_ref, routing_ref,
    res_hbm, q_hbm, k_hbm, v_hbm, w_hbm, router_hbm, gate_hbm, up_hbm, down_hbm,
    out_ref,
    res, q_raw, k_raw, v_raw, router, gate, up, down,
    kv_own, kv_all, w_own, w_all, q_rot, bias, rows_all, proj, got,
    x_out, arrived, stacked, back, returned, restacked,
    load_sems,
    kzs, kzr, kys, kyr, kcs, kcr, wzs, wzr, wys, wyr, wcs, wcr, own_sems, as_, ar, ps, pr,
    xs, xr, bs, br,
):
    sources = (k_hbm, v_hbm, w_hbm, q_hbm, res_hbm, router_hbm, gate_hbm, up_hbm, down_hbm)
    targets = (k_raw, v_raw, w_own, q_raw, res, router, gate, up, down)
    loads = [
        pltpu.make_async_copy(a, b, load_sems.at[i]) for i, (a, b) in enumerate(zip(sources, targets))
    ]
    for load in loads[:6]:
        load.start()

    me = lax.axis_index("seq")
    f_me = lax.axis_index("fsdp")
    z_count = seq_count // 4
    z, y, c = me // 4, lax.rem(me // 2, 2), lax.rem(me, 2)
    rows, key_count = bias.shape
    group_size = HEADS // KVH
    copies = seq_count // EXPERTS

    def spot(row):
        return jnp.where(row < HALF, span_ref[0, 2 * me], span_ref[0, 2 * me + 1]) * HALF + row % HALF

    lane = lax.broadcasted_iota(jnp.int32, (rows, 2 * HD), 1)
    place = spot(lax.broadcasted_iota(jnp.int32, (rows, 2 * HD), 0)).astype(jnp.float32)
    half = HD // 2
    frequency = jnp.exp(-jnp.log(rope_base) * (lane % half).astype(jnp.float32) / half)
    angles = place * frequency
    low = (lane % HD) < half
    cosine = jnp.cos(angles)
    sine = jnp.where(low, -jnp.sin(angles), jnp.sin(angles))

    def rotated(pair):
        x = pair.astype(jnp.float32)
        swapped = jnp.where(low, pltpu.roll(x, 2 * HD - half, 1), pltpu.roll(x, half, 1))
        return (x * cosine + swapped * sine).astype(jnp.bfloat16)

    loads[0].wait()
    loads[1].wait()
    for i in range(KVH // 2):
        kv_own[:, i * 2 * HD:(i + 1) * 2 * HD] = rotated(k_raw[:, i * 2 * HD:(i + 1) * 2 * HD])
    kv_own[:, KVH * HD:] = v_raw[...]

    def peer_of(side, dz, cc, sign=1):
        zz = lax.rem(z + dz, z_count) if sign > 0 else lax.rem(z + z_count - dz, z_count)
        return (zz * 2 + (1 - y if side else y)) * 2 + (1 - c if cc else c)

    relative = [(side, dz, cc) for side in range(2) for dz in range(z_count) for cc in range(2)]
    peers = [{"seq": peer_of(*r)} for r in relative[1:]]
    peers += [{"fsdp": lax.rem(f_me + d, fsdp_count)} for d in range(1, fsdp_count)]
    greet(peers)

    kv = gather_plan(kv_own, kv_all, (kzs, kzr, kys, kyr, kcs, kcr, own_sems.at[0]), z_count, z, y, c)
    w = gather_plan(w_own, w_all, (wzs, wzr, wys, wyr, wcs, wcr, own_sems.at[1]), z_count, z, y, c)
    kv[0]()
    kv[1](0)
    loads[2].wait()
    w[0]()
    loads[3].wait()
    for i in range(HEADS // 2):
        pair = rotated(q_raw[:, i * 2 * HD:(i + 1) * 2 * HD]) * jnp.bfloat16(HD ** -0.5)
        g, inside = (2 * i) // group_size, (2 * i) % group_size
        q_rot[g, inside * rows:(inside + 1) * rows, :] = pair[:, :HD]
        q_rot[g, (inside + 1) * rows:(inside + 2) * rows, :] = pair[:, HD:]
    key_row = lax.broadcasted_iota(jnp.int32, (1, key_count), 1)
    span_of_key = jnp.zeros((1, key_count), jnp.int32)
    for i in range(span_ref.shape[1]):
        span_of_key = jnp.where(key_row // HALF == i, span_ref[0, i], span_of_key)
    key_at = span_of_key * HALF + key_row % HALF
    query_at = spot(lax.broadcasted_iota(jnp.int32, (rows, 1), 0))
    bias[...] = jnp.where(key_at <= query_at, 0.0, masked_score)

    chosen = routing_ref[...]
    expert_row = lax.broadcasted_iota(jnp.int32, (EXPERTS, rows), 0)
    picks = [chosen[j:j + 1, :] == expert_row for j in range(TOPK)]
    named = sum(p.astype(jnp.float32) for p in picks)
    earlier = lax.broadcasted_iota(jnp.int32, (rows, rows), 0) < lax.broadcasted_iota(
        jnp.int32, (rows, rows), 1
    )
    before = jnp.dot(named, earlier.astype(jnp.float32), preferred_element_type=jnp.float32)
    slots = [
        jnp.sum(jnp.where(p, before, 0.0), axis=0, keepdims=True).astype(jnp.int32) for p in picks
    ]

    for d in range(1, z_count):
        kv[1](d)
    for d in range(z_count):
        kv[2](d)
    w[1](0)
    for load in loads[6:]:
        load.start()
    kv[3]()

    chunk = 4

    def send_rows(g):
        return [
            remote(
                rows_all.at[g, f_me], rows_all.at[g, f_me], as_.at[g, d], ar.at[g, d],
                fsdp=lax.rem(f_me + d, fsdp_count),
            )
            for d in range(1, fsdp_count)
        ]

    row_copies = [send_rows(g) for g in range(KVH)]
    relayed = 1
    for g in range(KVH):
        keys = kv_all[:, :, g * HD:(g + 1) * HD].reshape(key_count, HD)
        vals = kv_all[:, :, (KVH + g) * HD:(KVH + g + 1) * HD].reshape(key_count, HD)
        parts = []
        for part in range(group_size // chunk):
            q = q_rot[g, part * chunk * rows:(part + 1) * chunk * rows, :]
            s = lax.dot_general(q, keys, (((1,), (1,)), ((), ())), preferred_element_type=jnp.float32)
            weights, totals = [], []
            for i in range(chunk):
                sink = sink_ref[0, g * group_size + part * chunk + i]
                one = s[i * rows:(i + 1) * rows, :] + bias[...]
                top = jnp.maximum(jnp.max(one, axis=1, keepdims=True), sink)
                p = jnp.exp(one - top)
                totals.append(jnp.sum(p, axis=1, keepdims=True) + jnp.exp(sink - top))
                weights.append(p.astype(jnp.bfloat16))
            o = jnp.dot(jnp.concatenate(weights, axis=0), vals, preferred_element_type=jnp.float32)
            for i in range(chunk):
                parts.append((o[i * rows:(i + 1) * rows, :] / totals[i]).astype(jnp.bfloat16))
            if part == 0 and g > 0:
                for copy in row_copies[g - 1]:
                    copy.start()
        rows_all[g, pl.ds(f_me, 1)] = jnp.concatenate(parts, axis=1)[None]
        while relayed < z_count and relayed * KVH <= (g + 1) * z_count - KVH:
            w[1](relayed)
            relayed += 1
    for d in range(relayed, z_count):
        w[1](d)
    for copy in row_copies[KVH - 1]:
        copy.start()
    for d in range(z_count):
        w[2](d)
    loads[4].wait()
    loads[5].wait()
    w[3]()

    width = group_size * HD
    w_rows = w_own.shape[1]
    count = width // w_rows
    pair = max(1, 256 // w_rows)
    total = None
    for g in range(KVH):
        for copy in row_copies[g]:
            copy.wait_recv()
        for first in range(0, count, pair):
            block = jnp.concatenate([w_all[g * count + first + i] for i in range(pair)], axis=1)
            term = lax.dot_general(
                rows_all[g, :, :, first * w_rows:(first + pair) * w_rows].reshape(
                    fsdp_count * rows, pair * w_rows
                ),
                block, (((1,), (1,)), ((), ())), preferred_element_type=jnp.float32,
            )
            total = term if total is None else total + term
    proj[...] = total.astype(jnp.bfloat16).reshape(proj.shape)
    backs = []
    for d in range(1, fsdp_count):
        peer = lax.rem(f_me + d, fsdp_count)
        backs.append(remote(proj.at[peer], got.at[f_me], ps.at[d], pr.at[d], fsdp=peer))
    for copy in backs:
        copy.start()
    got[pl.ds(f_me, 1)] = proj[pl.ds(f_me, 1)]
    kv[4]()
    w[4]()
    for g in range(KVH):
        for copy in row_copies[g]:
            copy.wait_send()
    for copy in backs:
        copy.wait_recv()
    columns = w_own.shape[0]
    for f in range(fsdp_count):
        out_ref[0, :, f * columns:(f + 1) * columns] = got[f]
    for copy in backs:
        copy.wait_send()

    stream = res[...].astype(jnp.float32) + out_ref[0].astype(jnp.float32)
    normed = (
        stream
        * lax.rsqrt(jnp.mean(stream * stream, axis=-1, keepdims=True) + norm_eps)
        * gain_ref[...][None, :].astype(jnp.float32)
    ).astype(jnp.bfloat16)
    place = lax.broadcasted_iota(jnp.int32, (EXPERTS * CAP, rows), 0)
    dispatch = sum(
        (place == chosen[j:j + 1, :] * CAP + slots[j]).astype(jnp.float32) for j in range(TOPK)
    ).astype(jnp.bfloat16)
    buffer = jnp.dot(dispatch, normed, preferred_element_type=jnp.float32).astype(jnp.bfloat16)
    for e in range(EXPERTS):
        x_out[e] = buffer[e * CAP:(e + 1) * CAP, :]

    sends, returns = {}, {}
    for r, rel in enumerate(relative[1:], 1):
        to, source = peer_of(*rel), peer_of(*rel, sign=-1)
        sends[r] = remote(x_out.at[to // copies], arrived.at[r], xs.at[r], xr.at[r], seq=to)
        returns[r] = remote(back.at[r], returned.at[me], bs.at[r], br.at[r], seq=source)
    own = pltpu.make_async_copy(x_out.at[me // copies], arrived.at[0], own_sems.at[2])
    keep = pltpu.make_async_copy(back.at[0], returned.at[me], own_sems.at[3])
    for copy in sends.values():
        copy.start()
    own.start()

    logits = lax.dot_general(
        router[...], normed, (((1,), (1,)), ((), ())), preferred_element_type=jnp.float32
    )
    told = [jnp.sum(jnp.where(p, logits, 0.0), axis=0, keepdims=True) for p in picks]
    gates = [1.0 / sum(jnp.exp(t - told[j]) for t in told) for j in range(TOPK)]
    slot_row = lax.broadcasted_iota(jnp.int32, (seq_count * CAP, rows), 0)
    mixing = sum(
        jnp.where(
            (slot_row // (CAP * copies) == chosen[j:j + 1, :]) & (slot_row % CAP == slots[j]),
            gates[j],
            0.0,
        )
        for j in range(TOPK)
    )
    coarse = mixing.astype(jnp.bfloat16)
    fine = (mixing - coarse.astype(jnp.float32)).astype(jnp.bfloat16)

    for load in loads[6:]:
        load.wait()
    per_side = len(relative) // 2
    for side in range(2):
        for i in range(per_side):
            r = side * per_side + i
            sends[r].wait_recv() if r > 0 else own.wait()
            stacked[i * CAP:(i + 1) * CAP, :] = arrived[r]
        x = stacked[...]
        g = jnp.dot(x, gate[...], preferred_element_type=jnp.float32)
        u = jnp.dot(x, up[...], preferred_element_type=jnp.float32)
        hidden = (g * jax.nn.sigmoid(1.702 * g) * (u + 1.0)).astype(jnp.bfloat16)
        part = jnp.dot(hidden, down[...], preferred_element_type=jnp.float32).astype(jnp.bfloat16)
        for i in range(per_side):
            back[side * per_side + i] = part[i * CAP:(i + 1) * CAP, :]
        for i in range(per_side):
            r = side * per_side + i
            returns[r].start() if r > 0 else keep.start()
    for copy in sends.values():
        copy.wait_send()
    for copy in returns.values():
        copy.wait_recv()
    keep.wait()
    for i in range(seq_count):
        restacked[i * CAP:(i + 1) * CAP, :] = returned[i]
    outs = restacked[...]
    by_slot = (((0,), (0,)), ((), ()))
    mixed = lax.dot_general(coarse, outs, by_slot, preferred_element_type=jnp.float32) + lax.dot_general(
        fine, outs, by_slot, preferred_element_type=jnp.float32
    )
    out_ref[1] = (res[...].astype(jnp.float32) + out_ref[0].astype(jnp.float32) + mixed).astype(jnp.bfloat16)
    for copy in returns.values():
        copy.wait_send()


def on_device(
    residual,
    queries,
    key_rows,
    values,
    attention_sinks,
    out_weight,
    norm_gain,
    router_weight,
    gate_weight,
    up_weight,
    down_weight,
    routing,
    span_order,
):
    seq_count = lax.axis_size("seq")
    fsdp_count = lax.axis_size("fsdp")
    z_count = seq_count // 4
    rows = residual.shape[1]
    dma = pltpu.SemaphoreType.DMA
    vmem = pl.BlockSpec(memory_space=pltpu.VMEM)
    smem = pl.BlockSpec(memory_space=pltpu.SMEM)
    hbm = pl.BlockSpec(memory_space=pl.ANY)
    gather_sems = [dma((z_count,))] * 4 + [dma((2, z_count))] * 2

    def held(*shape):
        return pltpu.VMEM(shape, jnp.bfloat16)

    kv_width = 2 * KVH * HD
    w_rows, columns = out_weight.shape
    both = pl.pallas_call(
        functools.partial(layer_kernel, seq_count, fsdp_count),
        out_shape=jax.ShapeDtypeStruct((2, rows, D), jnp.bfloat16),
        in_specs=[smem, smem, vmem, vmem] + [hbm] * 9,
        out_specs=vmem,
        scratch_shapes=[
            held(rows, D),
            held(rows, HEADS * HD),
            held(rows, KVH * HD),
            held(rows, KVH * HD),
            held(*router_weight.shape[::-1]),
            held(*gate_weight.shape),
            held(*up_weight.shape),
            held(*down_weight.shape),
            held(rows, kv_width),
            held(seq_count, rows, kv_width),
            held(columns, w_rows),
            held(seq_count, columns, w_rows),
            held(KVH, HEADS // KVH * rows, HD),
            pltpu.VMEM((rows, seq_count * rows), jnp.float32),
            held(KVH, fsdp_count, rows, HEADS // KVH * HD),
            held(fsdp_count, rows, columns),
            held(fsdp_count, rows, columns),
            held(EXPERTS, CAP, D),
            held(seq_count, CAP, D),
            held(seq_count // 2 * CAP, D),
            held(seq_count, CAP, D),
            held(seq_count, CAP, D),
            held(seq_count * CAP, D),
            dma((9,)),
        ]
        + gather_sems
        + gather_sems
        + [dma((4,)), dma((KVH, fsdp_count)), dma((KVH, fsdp_count)), dma((fsdp_count,)), dma((fsdp_count,))]
        + [dma((seq_count,))] * 4,
        compiler_params=pltpu.CompilerParams(
            collective_id=0, has_side_effects=True, vmem_limit_bytes=60 * 1024 * 1024
        ),
    )(
        attention_sinks[None, :],
        span_order[None, :],
        norm_gain,
        routing[0].T,
        residual[0],
        queries[0],
        key_rows[0],
        values[0],
        out_weight.T,
        router_weight.T,
        gate_weight,
        up_weight,
        down_weight,
    )
    return (both[0][None], both[1][None])


def solution(mesh):
    in_specs = (
        P("fsdp", "seq", None),
        P("fsdp", "seq", None),
        P("fsdp", "seq", None),
        P("fsdp", "seq", None),
        P(),
        P("seq", "fsdp"),
        P(),
        P(),
        P(None, "seq"),
        P(None, "seq"),
        P("seq", None),
        P("fsdp", "seq", None),
        P(),
    )
    out_specs = (P("fsdp", "seq", None), P("fsdp", "seq", None))
    return jax.shard_map(
        on_device, mesh=mesh, in_specs=in_specs, out_specs=out_specs, check_vma=False
    )
```

```python
import functools

import jax
import jax.numpy as jnp
from jax import lax
from jax.experimental import pallas as pl
from jax.experimental.pallas import tpu as pltpu
from jax.sharding import PartitionSpec as P

D = 1440
HEADS = 32
KVH = 4
HD = 64
EXPERTS = 16
TOPK = 2
TOK_DEV = 64
HALF = 32
CAP = 12


rope_base = 150000.0
norm_eps = 1e-05
masked_score = -1e30


MESH = pl.DeviceIdType.MESH


def remote(source, target, send_sem, recv_sem, **where):
    return pltpu.make_async_remote_copy(
        src_ref=source,
        dst_ref=target,
        send_sem=send_sem,
        recv_sem=recv_sem,
        device_id=where,
        device_id_type=MESH,
    )


def greet(peers):
    barrier = pltpu.get_barrier_semaphore()
    for where in peers:
        pl.semaphore_signal(barrier, inc=1, device_id=where, device_id_type=MESH)
    pl.semaphore_wait(barrier, len(peers))


def slot(z, y, c):
    return (z * 2 + y) * 2 + c


def gather_plan(slots, sems, z_count, z, y, c):
    z_send, z_recv, y_send, y_recv, c_send, c_recv = sems

    def z_of(d):
        return lax.rem(z + z_count - d, z_count)

    own = slots.at[slot(z, y, c)]
    to_z = [
        remote(own, own, z_send.at[d], z_recv.at[d], seq=slot(lax.rem(z + d, z_count), y, c))
        for d in range(1, z_count)
    ]

    def to_y(d):
        block = slots.at[slot(z_of(d), y, c)]
        return remote(block, block, y_send.at[d], y_recv.at[d], seq=slot(z, 1 - y, c))

    def to_c(side, d):
        block = slots.at[slot(z_of(d), y if side == 0 else 1 - y, c)]
        return remote(block, block, c_send.at[side, d], c_recv.at[side, d], seq=slot(z, y, 1 - c))

    ys = [to_y(d) for d in range(z_count)]
    cs = [[to_c(side, d) for d in range(z_count)] for side in range(2)]

    def start_z():
        for copy in to_z:
            copy.start()

    def relay(d):
        if d > 0:
            to_z[d - 1].wait_recv()
        ys[d].start()
        cs[0][d].start()

    def relay_across(d):
        ys[d].wait_recv()
        cs[1][d].start()

    def finish():
        for side in range(2):
            for d in range(z_count):
                cs[side][d].wait_recv()

    def drain():
        for copy in to_z + ys + cs[0] + cs[1]:
            copy.wait_send()

    return start_z, relay, relay_across, finish, drain


def line_plan(slots, pieces, sems, z_count, z, y, c):
    z_send, z_recv, y_send, y_recv, c_send, c_recv = sems
    last = z_count - 1

    def block(zz, yy, p):
        return slots.at[slot(zz, yy, c), pl.ds(*pieces[p])]

    def along(way, zz, p):
        part = block(zz, y, p)
        return remote(part, part, z_send.at[way, zz, p], z_recv.at[zz, p], seq=slot(z + 1 - 2 * way, y, c))

    def over(zz, p):
        part = block(zz, y, p)
        return remote(part, part, y_send.at[zz, p], y_recv.at[zz, p], seq=slot(z, 1 - y, c))

    def beside(side, zz, p):
        part = block(zz, 1 - y if side else y, p)
        return remote(part, part, c_send.at[side, zz, p], c_recv.at[side, zz, p], seq=slot(z, y, 1 - c))

    def onward(way, zz, p):
        @pl.when(z < last if way == 0 else z > 0)
        def _():
            along(way, zz, p).start()

    def start(p):
        onward(0, z, p)
        onward(1, z, p)
        over(z, p).start()
        beside(0, z, p).start()

    def each(k, act):
        for way in range(2):
            zz = z - 1 - k if way == 0 else z + 1 + k

            @pl.when(zz >= 0 if way == 0 else zz <= last)
            def _(way=way, zz=zz):
                act(way, zz)

    def relay(k, p):
        def act(way, zz):
            along(way, zz, p).wait_recv()
            onward(way, zz, p)
            over(zz, p).start()
            beside(0, zz, p).start()

        each(k, act)

    def across(k, p):
        def act(way, zz):
            over(zz, p).wait_recv()
            beside(1, zz, p).start()

        if k < 0:
            act(0, z)
        else:
            each(k, act)

    every = [(zz, p) for zz in range(z_count) for p in range(len(pieces))]

    def finish():
        for zz, p in every:
            for side in range(2):
                beside(side, zz, p).wait_recv()

    def drain():
        for zz, p in every:
            @pl.when((z >= zz) & (z < last))
            def _():
                along(0, zz, p).wait_send()

            @pl.when((z <= zz) & (z > 0))
            def _():
                along(1, zz, p).wait_send()

            over(zz, p).wait_send()
            for side in range(2):
                beside(side, zz, p).wait_send()

    return start, relay, across, finish, drain


def layer_kernel(
    seq_count, fsdp_count,
    sink_ref, span_ref, gain_ref, routing_ref,
    res_hbm, q_hbm, k_hbm, v_hbm, w_hbm, router_hbm, gate_hbm, up_hbm, down_hbm,
    out_ref,
    res, q_raw, k_raw, v_raw, router, gate, up, down,
    kv_all, w_all, q_rot, bias, rows_all, proj, got,
    x_out, arrived, stacked, back, returned, mix,
    load_sems,
    kzs, kzr, kys, kyr, kcs, kcr, wzs, wzr, wys, wyr, wcs, wcr, own_sems, as_, ar, ps, pr,
    xs, xr, bs, br,
):
    me = lax.axis_index("seq")
    f_me = lax.axis_index("fsdp")
    sources = (k_hbm, v_hbm, w_hbm, q_hbm, res_hbm, router_hbm, gate_hbm, up_hbm, down_hbm)
    targets = (k_raw, v_raw, w_all.at[me], q_raw, res, router, gate, up, down)
    loads = [
        pltpu.make_async_copy(a, b, load_sems.at[i]) for i, (a, b) in enumerate(zip(sources, targets))
    ]
    for load in loads[:6]:
        load.start()

    z_count = seq_count // 4
    z, y, c = me // 4, lax.rem(me // 2, 2), lax.rem(me, 2)
    rows, key_count = bias.shape
    group_size = HEADS // KVH
    copies = seq_count // EXPERTS

    def spot(row):
        return jnp.where(row < HALF, span_ref[0, 2 * me], span_ref[0, 2 * me + 1]) * HALF + row % HALF

    lane = lax.broadcasted_iota(jnp.int32, (rows, 2 * HD), 1)
    place = spot(lax.broadcasted_iota(jnp.int32, (rows, 2 * HD), 0)).astype(jnp.float32)
    half = HD // 2
    frequency = jnp.exp(-jnp.log(rope_base) * (lane % half).astype(jnp.float32) / half)
    angles = place * frequency
    low = (lane % HD) < half
    cosine = jnp.cos(angles)
    sine = jnp.where(low, -jnp.sin(angles), jnp.sin(angles))

    def rotated(pair):
        x = pair.astype(jnp.float32)
        swapped = jnp.where(low, pltpu.roll(x, 2 * HD - half, 1), pltpu.roll(x, half, 1))
        return (x * cosine + swapped * sine).astype(jnp.bfloat16)

    loads[0].wait()
    loads[1].wait()
    keys = [rotated(k_raw[:, i * 2 * HD:(i + 1) * 2 * HD]) for i in range(KVH // 2)]
    kv_all[pl.ds(me, 1)] = jnp.concatenate(keys + [v_raw[...]], axis=1)[None]

    reach = z_count // 2
    base, inner = z // reach, lax.rem(z, reach)

    def peer_of(far, j, side, cc, sign=1):
        step = lax.rem(inner + j, reach) if sign > 0 else lax.rem(inner + reach - j, reach)
        zz = (1 - base if far else base) * reach + step
        return (zz * 2 + (1 - y if side else y)) * 2 + (1 - c if cc else c)

    relative = [
        (far, j, side, cc) for far in range(2) for j in range(reach) for side in range(2) for cc in range(2)
    ]
    peers = [{"seq": peer_of(*r)} for r in relative[1:]]
    peers += [{"fsdp": lax.rem(f_me + d, fsdp_count)} for d in range(1, fsdp_count)]
    greet(peers)

    w_columns, w_rows = w_all.shape[1:]
    cut = w_columns // 32 * 16
    pieces = [(0, cut), (cut, w_columns - cut)] if w_columns % 16 == 0 else [(0, w_columns)]
    kv = gather_plan(kv_all, (kzs, kzr, kys, kyr, kcs, kcr), z_count, z, y, c)
    w = line_plan(w_all, pieces, (wzs, wzr, wys, wyr, wcs, wcr), z_count, z, y, c)
    kv[0]()
    kv[1](0)
    loads[2].wait()
    for p in range(len(pieces)):
        w[0](p)
    loads[3].wait()
    for i in range(HEADS // 2):
        pair = rotated(q_raw[:, i * 2 * HD:(i + 1) * 2 * HD]) * jnp.bfloat16(HD ** -0.5)
        g, inside = (2 * i) // group_size, (2 * i) % group_size
        q_rot[g, inside * rows:(inside + 1) * rows, :] = pair[:, :HD]
        q_rot[g, (inside + 1) * rows:(inside + 2) * rows, :] = pair[:, HD:]
    key_row = lax.broadcasted_iota(jnp.int32, (1, key_count), 1)
    span_of_key = jnp.zeros((1, key_count), jnp.int32)
    for i in range(span_ref.shape[1]):
        span_of_key = jnp.where(key_row // HALF == i, span_ref[0, i], span_of_key)
    key_at = span_of_key * HALF + key_row % HALF
    query_at = spot(lax.broadcasted_iota(jnp.int32, (rows, 1), 0))
    bias[...] = jnp.where(key_at <= query_at, 0.0, masked_score)

    chosen = routing_ref[...]
    expert_row = lax.broadcasted_iota(jnp.int32, (EXPERTS, rows), 0)
    picks = [chosen[j:j + 1, :] == expert_row for j in range(TOPK)]
    named = sum(p.astype(jnp.float32) for p in picks)
    earlier = lax.broadcasted_iota(jnp.int32, (rows, rows), 0) < lax.broadcasted_iota(
        jnp.int32, (rows, rows), 1
    )
    before = jnp.dot(named, earlier.astype(jnp.float32), preferred_element_type=jnp.float32)
    slots = [
        jnp.sum(jnp.where(p, before, 0.0), axis=0, keepdims=True).astype(jnp.int32) for p in picks
    ]

    for d in range(1, z_count):
        kv[1](d)
    for load in loads[6:]:
        load.start()
    steps = [functools.partial(w[1], 0, p) for p in range(len(pieces))]
    steps += [functools.partial(w[2], -1, p) for p in range(len(pieces))]
    for k in range(1, z_count - 1):
        for p in range(len(pieces)):
            steps += [functools.partial(w[1], k, p), functools.partial(w[2], k - 1, p)]
    closing = [functools.partial(w[2], z_count - 2, p) for p in range(len(pieces))]
    early = len(pieces)
    steps.pop(0)()
    for d in range(z_count):
        kv[2](d)
    for _ in range(early - 1):
        steps.pop(0)()
    kv[3]()

    chunk = 4

    def send_rows(g):
        return [
            remote(
                rows_all.at[g, f_me], rows_all.at[g, f_me], as_.at[g, d], ar.at[g, d],
                fsdp=lax.rem(f_me + d, fsdp_count),
            )
            for d in range(1, fsdp_count)
        ]

    row_copies = [send_rows(g) for g in range(KVH)]
    turns = KVH * group_size // chunk
    share = -(-len(steps) // turns)
    for g in range(KVH):
        keys = kv_all[:, :, g * HD:(g + 1) * HD].reshape(key_count, HD)
        vals = kv_all[:, :, (KVH + g) * HD:(KVH + g + 1) * HD].reshape(key_count, HD)
        parts = []
        for part in range(group_size // chunk):
            q = q_rot[g, part * chunk * rows:(part + 1) * chunk * rows, :]
            s = lax.dot_general(q, keys, (((1,), (1,)), ((), ())), preferred_element_type=jnp.float32)
            weights, totals = [], []
            for i in range(chunk):
                sink = sink_ref[0, g * group_size + part * chunk + i]
                one = s[i * rows:(i + 1) * rows, :] + bias[...]
                top = jnp.maximum(jnp.max(one, axis=1, keepdims=True), sink)
                p = jnp.exp(one - top)
                totals.append(jnp.sum(p, axis=1, keepdims=True) + jnp.exp(sink - top))
                weights.append(p.astype(jnp.bfloat16))
            o = jnp.dot(jnp.concatenate(weights, axis=0), vals, preferred_element_type=jnp.float32)
            for i in range(chunk):
                parts.append((o[i * rows:(i + 1) * rows, :] / totals[i]).astype(jnp.bfloat16))
            if part == 0 and g > 0:
                for copy in row_copies[g - 1]:
                    copy.start()
            for step in steps[:share]:
                step()
            steps = steps[share:]
        rows_all[g, pl.ds(f_me, 1)] = jnp.concatenate(parts, axis=1)[None]
    for copy in row_copies[KVH - 1]:
        copy.start()
    for step in steps + closing:
        step()
    loads[4].wait()
    loads[5].wait()
    w[3]()

    width = group_size * HD
    count = width // w_rows
    pair = max(1, 256 // w_rows)
    total = None
    for g in range(KVH):
        for copy in row_copies[g]:
            copy.wait_recv()
        for first in range(0, count, pair):
            block = jnp.concatenate([w_all[g * count + first + i] for i in range(pair)], axis=1)
            term = lax.dot_general(
                rows_all[g, :, :, first * w_rows:(first + pair) * w_rows].reshape(
                    fsdp_count * rows, pair * w_rows
                ),
                block, (((1,), (1,)), ((), ())), preferred_element_type=jnp.float32,
            )
            total = term if total is None else total + term
    proj[...] = total.astype(jnp.bfloat16).reshape(proj.shape)
    backs = []
    for d in range(1, fsdp_count):
        peer = lax.rem(f_me + d, fsdp_count)
        backs.append(remote(proj.at[peer], got.at[f_me], ps.at[d], pr.at[d], fsdp=peer))
    for copy in backs:
        copy.start()
    got[pl.ds(f_me, 1)] = proj[pl.ds(f_me, 1)]
    kv[4]()
    w[4]()
    for g in range(KVH):
        for copy in row_copies[g]:
            copy.wait_send()
    for copy in backs:
        copy.wait_recv()
    for f in range(fsdp_count):
        out_ref[0, :, f * w_columns:(f + 1) * w_columns] = got[f]
    for copy in backs:
        copy.wait_send()

    stream = res[...].astype(jnp.float32) + out_ref[0].astype(jnp.float32)
    normed = (
        stream
        * lax.rsqrt(jnp.mean(stream * stream, axis=-1, keepdims=True) + norm_eps)
        * gain_ref[...][None, :].astype(jnp.float32)
    ).astype(jnp.bfloat16)
    fold = x_out.shape[2]
    spare = 2 * fold - D
    column = lax.broadcasted_iota(jnp.int32, (1, 2 * rows), 1)
    wrap = column // rows
    chosen_twice = jnp.concatenate([chosen, chosen], axis=1)
    slot_twice = [jnp.concatenate([slots[j], slots[j]], axis=1) for j in range(TOPK)]
    place = lax.broadcasted_iota(jnp.int32, (EXPERTS * 2 * CAP, 2 * rows), 0)
    dispatch = sum(
        (place == chosen_twice[j:j + 1, :] * (2 * CAP) + wrap * CAP + slot_twice[j]).astype(jnp.float32)
        for j in range(TOPK)
    ).astype(jnp.bfloat16)

    def folded(wide):
        right = jnp.concatenate([wide[:, fold:], jnp.zeros((wide.shape[0], spare), wide.dtype)], axis=1)
        return wide[:, :fold], right

    buffer = jnp.dot(
        dispatch, jnp.concatenate(folded(normed), axis=0), preferred_element_type=jnp.float32
    ).astype(jnp.bfloat16)
    for e in range(EXPERTS):
        x_out[e] = buffer[e * 2 * CAP:(e + 1) * 2 * CAP, :]

    sends, returns = {}, {}
    for r, rel in enumerate(relative[1:], 1):
        to, source = peer_of(*rel), peer_of(*rel, sign=-1)
        sends[r] = remote(x_out.at[to // copies], arrived.at[r], xs.at[r], xr.at[r], seq=to)
        returns[r] = remote(back.at[r], returned.at[me], bs.at[r], br.at[r], seq=source)
    own = pltpu.make_async_copy(x_out.at[me // copies], arrived.at[0], own_sems.at[2])
    keep = pltpu.make_async_copy(back.at[0], returned.at[me], own_sems.at[3])
    for copy in sends.values():
        copy.start()
    own.start()

    logits = lax.dot_general(
        router[...], normed, (((1,), (1,)), ((), ())), preferred_element_type=jnp.float32
    )
    told = [jnp.sum(jnp.where(p, logits, 0.0), axis=0, keepdims=True) for p in picks]
    gates = [1.0 / sum(jnp.exp(t - told[j]) for t in told) for j in range(TOPK)]
    slot_row = lax.broadcasted_iota(jnp.int32, (seq_count * 2 * CAP, 2 * rows), 0)
    within = slot_row % (2 * CAP)
    mixing = sum(
        jnp.where(
            (slot_row // (2 * CAP * copies) == chosen_twice[j:j + 1, :])
            & (within == wrap * CAP + slot_twice[j]),
            jnp.concatenate([gates[j], gates[j]], axis=1),
            0.0,
        )
        for j in range(TOPK)
    )
    coarse = mixing.astype(jnp.bfloat16).astype(jnp.float32)
    mix[...] = jnp.concatenate([coarse, mixing - coarse], axis=1).T.astype(jnp.bfloat16)

    for load in loads[6:]:
        load.wait()
    near = len(relative) // 2
    chunks = [range(near), range(near, near + near // 2), range(near + near // 2, 2 * near)]
    for chunk in chunks:
        for i, r in enumerate(chunk):
            sends[r].wait_recv() if r > 0 else own.wait()
            block = arrived[r]
            stacked[i * CAP:(i + 1) * CAP, :fold] = block[:CAP, :]
            stacked[i * CAP:(i + 1) * CAP, fold:] = block[CAP:, :D - fold]
        x = stacked[:len(chunk) * CAP, :]
        g = jnp.dot(x, gate[...], preferred_element_type=jnp.float32)
        u = jnp.dot(x, up[...], preferred_element_type=jnp.float32)
        hidden = (g * jax.nn.sigmoid(1.702 * g) * (u + 1.0)).astype(jnp.bfloat16)
        part = jnp.dot(hidden, down[...], preferred_element_type=jnp.float32).astype(jnp.bfloat16)
        left, right = folded(part)
        for i, r in enumerate(chunk):
            back[r, :CAP] = left[i * CAP:(i + 1) * CAP, :]
            back[r, CAP:] = right[i * CAP:(i + 1) * CAP, :]
        for r in chunk:
            returns[r].start() if r > 0 else keep.start()
    for copy in sends.values():
        copy.wait_send()
    for copy in returns.values():
        copy.wait_recv()
    keep.wait()
    parts = jnp.dot(
        mix[...], returned[...].reshape(seq_count * 2 * CAP, fold), preferred_element_type=jnp.float32
    )
    mixed = [parts[h * rows:(h + 1) * rows, :] + parts[(2 + h) * rows:(3 + h) * rows, :] for h in range(2)]
    stream = res[...].astype(jnp.float32) + out_ref[0].astype(jnp.float32)
    out_ref[1, :, :fold] = (stream[:, :fold] + mixed[0]).astype(jnp.bfloat16)
    out_ref[1, :, fold:] = (stream[:, fold:] + mixed[1][:, :D - fold]).astype(jnp.bfloat16)
    for copy in returns.values():
        copy.wait_send()


def on_device(
    residual,
    queries,
    key_rows,
    values,
    attention_sinks,
    out_weight,
    norm_gain,
    router_weight,
    gate_weight,
    up_weight,
    down_weight,
    routing,
    span_order,
):
    seq_count = lax.axis_size("seq")
    fsdp_count = lax.axis_size("fsdp")
    z_count = seq_count // 4
    rows = residual.shape[1]
    dma = pltpu.SemaphoreType.DMA
    vmem = pl.BlockSpec(memory_space=pltpu.VMEM)
    smem = pl.BlockSpec(memory_space=pltpu.SMEM)
    hbm = pl.BlockSpec(memory_space=pl.ANY)

    def held(*shape):
        return pltpu.VMEM(shape, jnp.bfloat16)

    kv_width = 2 * KVH * HD
    fold = -(-D // 256) * 128
    w_rows, columns = out_weight.shape
    both = pl.pallas_call(
        functools.partial(layer_kernel, seq_count, fsdp_count),
        out_shape=jax.ShapeDtypeStruct((2, rows, D), jnp.bfloat16),
        in_specs=[smem, smem, vmem, vmem] + [hbm] * 9,
        out_specs=vmem,
        scratch_shapes=[
            held(rows, D),
            held(rows, HEADS * HD),
            held(rows, KVH * HD),
            held(rows, KVH * HD),
            held(*router_weight.shape[::-1]),
            held(*gate_weight.shape),
            held(*up_weight.shape),
            held(*down_weight.shape),
            held(seq_count, rows, kv_width),
            held(seq_count, columns, w_rows),
            held(KVH, HEADS // KVH * rows, HD),
            pltpu.VMEM((rows, seq_count * rows), jnp.float32),
            held(KVH, fsdp_count, rows, HEADS // KVH * HD),
            held(fsdp_count, rows, columns),
            held(fsdp_count, rows, columns),
            held(EXPERTS, 2 * CAP, fold),
            held(seq_count, 2 * CAP, fold),
            held(seq_count // 2 * CAP, D),
            held(seq_count, 2 * CAP, fold),
            held(seq_count, 2 * CAP, fold),
            held(4 * rows, seq_count * 2 * CAP),
            dma((9,)),
        ]
        + [dma((z_count,))] * 4
        + [dma((2, z_count))] * 2
        + [dma((2, z_count, 2)), dma((z_count, 2)), dma((z_count, 2)), dma((z_count, 2))]
        + [dma((2, z_count, 2))] * 2
        + [dma((4,)), dma((KVH, fsdp_count)), dma((KVH, fsdp_count)), dma((fsdp_count,)), dma((fsdp_count,))]
        + [dma((seq_count,))] * 4,
        compiler_params=pltpu.CompilerParams(
            collective_id=0, has_side_effects=True, vmem_limit_bytes=60 * 1024 * 1024
        ),
    )(
        attention_sinks[None, :],
        span_order[None, :],
        norm_gain,
        routing[0].T,
        residual[0],
        queries[0],
        key_rows[0],
        values[0],
        out_weight.T,
        router_weight.T,
        gate_weight,
        up_weight,
        down_weight,
    )
    return (both[0][None], both[1][None])


def solution(mesh):
    in_specs = (
        P("fsdp", "seq", None),
        P("fsdp", "seq", None),
        P("fsdp", "seq", None),
        P("fsdp", "seq", None),
        P(),
        P("seq", "fsdp"),
        P(),
        P(),
        P(None, "seq"),
        P(None, "seq"),
        P("seq", None),
        P("fsdp", "seq", None),
        P(),
    )
    out_specs = (P("fsdp", "seq", None), P("fsdp", "seq", None))
    return jax.shard_map(
        on_device, mesh=mesh, in_specs=in_specs, out_specs=out_specs, check_vma=False
    )
```

```python
import functools

import jax
import jax.numpy as jnp
from jax import lax
from jax.experimental import pallas as pl
from jax.experimental.pallas import tpu as pltpu
from jax.sharding import PartitionSpec as P

D = 1440
HEADS = 32
KVH = 4
HD = 64
EXPERTS = 16
TOPK = 2
TOK_DEV = 64
HALF = 32
CAP = 12


rope_base = 150000.0
norm_eps = 1e-05
masked_score = -1e30


MESH = pl.DeviceIdType.MESH


def remote(source, target, send_sem, recv_sem, **where):
    return pltpu.make_async_remote_copy(
        src_ref=source,
        dst_ref=target,
        send_sem=send_sem,
        recv_sem=recv_sem,
        device_id=where,
        device_id_type=MESH,
    )


def slot(z, y, c):
    return (z * 2 + y) * 2 + c


def plane(far, j, z, z_count, sign=1):
    reach = z_count // 2
    base, inner = z // reach, lax.rem(z, reach)
    step = lax.rem(inner + j, reach) if sign > 0 else lax.rem(inner + reach - j, reach)
    return (1 - base if far else base) * reach + step


def gather_plan(slots, sems, z_count, z, y, c):
    z_send, z_recv, y_send, y_recv, c_send, c_recv = sems
    reach = z_count // 2
    order = [(0, 0)] + [(1, j) for j in range(reach)] + [(0, j) for j in range(1, reach)]

    def z_of(d):
        return plane(*order[d], z, z_count, sign=-1)

    own = slots.at[slot(z, y, c)]
    to_z = [
        remote(own, own, z_send.at[d], z_recv.at[d], seq=slot(plane(*order[d], z, z_count), y, c))
        for d in range(1, z_count)
    ]

    def to_y(d):
        block = slots.at[slot(z_of(d), y, c)]
        return remote(block, block, y_send.at[d], y_recv.at[d], seq=slot(z, 1 - y, c))

    def to_c(side, d):
        block = slots.at[slot(z_of(d), y if side == 0 else 1 - y, c)]
        return remote(block, block, c_send.at[side, d], c_recv.at[side, d], seq=slot(z, y, 1 - c))

    ys = [to_y(d) for d in range(z_count)]
    cs = [[to_c(side, d) for d in range(z_count)] for side in range(2)]

    def start_z():
        for copy in to_z:
            copy.start()

    def relay(d):
        if d > 0:
            to_z[d - 1].wait_recv()
        ys[d].start()
        cs[0][d].start()

    def relay_across(d):
        ys[d].wait_recv()
        cs[1][d].start()

    def finish():
        for side in range(2):
            for d in range(z_count):
                cs[side][d].wait_recv()

    def drain():
        for copy in to_z + ys + cs[0] + cs[1]:
            copy.wait_send()

    return start_z, relay, relay_across, finish, drain


def line_plan(slots, pieces, sems, z_count, z, y, c):
    z_send, z_recv, y_send, y_recv, c_send, c_recv = sems
    last = z_count - 1

    def block(side, zz, p):
        start, size, _ = pieces[p]
        return slots.at[slot(zz, 1 - y if side else y, c), pl.ds(start, size)]

    def along(way, side, zz, p):
        part = block(side, zz, p)
        return remote(
            part, part, z_send.at[way, side, zz, p], z_recv.at[side, zz, p], seq=slot(z + 1 - 2 * way, y, c)
        )

    def over(zz, p):
        part = block(0, zz, p)
        return remote(part, part, y_send.at[zz, p], y_recv.at[zz, p], seq=slot(z, 1 - y, c))

    def beside(side, zz, p):
        part = block(side, zz, p)
        return remote(part, part, c_send.at[side, zz, p], c_recv.at[side, zz, p], seq=slot(z, y, 1 - c))

    def sides(p):
        return range(2) if pieces[p][2] else range(1)

    def onward(way, side, zz, p):
        @pl.when(z < last if way == 0 else z > 0)
        def _():
            along(way, side, zz, p).start()

    def start(p):
        onward(0, 0, z, p)
        onward(1, 0, z, p)
        beside(0, z, p).start()

    def cross(p):
        over(z, p).start()

    def each(k, act):
        for way in range(2):
            zz = z - 1 - k if way == 0 else z + 1 + k

            @pl.when(zz >= 0 if way == 0 else zz <= last)
            def _(way=way, zz=zz):
                act(way, zz)

    def relay(k, p):
        def act(way, zz):
            for side in sides(p):
                along(way, side, zz, p).wait_recv()
                onward(way, side, zz, p)
                beside(side, zz, p).start()
            if not pieces[p][2]:
                over(zz, p).start()

        each(k, act)

    def across(k, p):
        def act(way, zz):
            over(zz, p).wait_recv()
            beside(1, zz, p).start()
            if pieces[p][2]:
                onward(0, 1, zz, p)
                onward(1, 1, zz, p)

        if k < 0:
            act(0, z)
        else:
            each(k, act)

    def ready(zz):
        for p in range(len(pieces)):
            for side in range(2):
                beside(side, zz, p).wait_recv()

    def drain():
        for p in range(len(pieces)):
            for zz in range(z_count):
                for side in sides(p):
                    @pl.when((z >= zz) & (z < last))
                    def _():
                        along(0, side, zz, p).wait_send()

                    @pl.when((z <= zz) & (z > 0))
                    def _():
                        along(1, side, zz, p).wait_send()

                if not pieces[p][2]:
                    over(zz, p).wait_send()
                for side in range(2):
                    beside(side, zz, p).wait_send()
            if pieces[p][2]:
                over(z, p).wait_send()

    return start, cross, relay, across, ready, drain


def layer_kernel(
    seq_count, fsdp_count,
    sink_hbm, span_hbm, gain_hbm, routing_hbm, res_hbm, q_hbm, k_hbm, v_hbm, w_hbm, router_hbm, gate_hbm, up_hbm, down_hbm,
    out_ref,
    sink_ref, span_ref, gain_ref, routing_ref, res, q_raw, k_raw, v_raw, router, gate, up, down,
    kv_all, w_all, q_rot, bias, rows_all, proj, got,
    x_out, arrived, stacked, back, returned, mix, dispatch,
    load_sems,
    kzs, kzr, kys, kyr, kcs, kcr, wzs, wzr, wys, wyr, wcs, wcr, as_, ar, ps, pr,
    xs, xr, bs, br,
):
    me = lax.axis_index("seq")
    f_me = lax.axis_index("fsdp")
    sources = (
        k_hbm, v_hbm, w_hbm, q_hbm, res_hbm, router_hbm, gate_hbm, up_hbm, down_hbm,
        span_hbm, sink_hbm, routing_hbm, gain_hbm,
    )
    targets = (
        k_raw, v_raw, w_all.at[me], q_raw, res, router, gate, up, down, span_ref, sink_ref, routing_ref, gain_ref,
    )
    loads = [
        pltpu.make_async_copy(a, b, load_sems.at[i]) for i, (a, b) in enumerate(zip(sources, targets))
    ]
    for load in loads[9:] + loads[:6]:
        load.start()

    z_count = seq_count // 4
    z, y, c = me // 4, lax.rem(me // 2, 2), lax.rem(me, 2)
    reach = z_count // 2

    def peer_of(far, j, side, cc, sign=1):
        zz = plane(far, j, z, z_count, sign)
        return (zz * 2 + (1 - y if side else y)) * 2 + (1 - c if cc else c)

    relative = [
        (far, j, side, cc) for far in range(2) for j in range(reach) for side in range(2) for cc in range(2)
    ]
    peers = [{"seq": peer_of(*r)} for r in relative[1:]]
    peers += [{"fsdp": lax.rem(f_me + d, fsdp_count)} for d in range(1, fsdp_count)]
    barrier = pltpu.get_barrier_semaphore()
    for where in peers:
        pl.semaphore_signal(barrier, inc=1, device_id=where, device_id_type=MESH)

    rows, key_count = bias.shape
    group_size = HEADS // KVH
    copies = seq_count // EXPERTS

    loads[9].wait()

    def spot(row):
        return jnp.where(row < HALF, span_ref[0, 2 * me], span_ref[0, 2 * me + 1]) * HALF + row % HALF

    lane = lax.broadcasted_iota(jnp.int32, (rows, 2 * HD), 1)
    place = spot(lax.broadcasted_iota(jnp.int32, (rows, 2 * HD), 0)).astype(jnp.float32)
    half = HD // 2
    frequency = jnp.exp(-jnp.log(rope_base) * (lane % half).astype(jnp.float32) / half)
    angles = place * frequency
    low = (lane % HD) < half
    cosine = jnp.cos(angles)
    sine = jnp.where(low, -jnp.sin(angles), jnp.sin(angles))

    def rotated(pair):
        x = pair.astype(jnp.float32)
        swapped = jnp.where(low, pltpu.roll(x, 2 * HD - half, 1), pltpu.roll(x, half, 1))
        return (x * cosine + swapped * sine).astype(jnp.bfloat16)

    loads[0].wait()
    loads[1].wait()
    keys = [rotated(k_raw[:, i * 2 * HD:(i + 1) * 2 * HD]) for i in range(KVH // 2)]
    kv_all[pl.ds(me, 1)] = jnp.concatenate(keys + [v_raw[...]], axis=1)[None]

    pl.semaphore_wait(barrier, len(peers))

    w_columns, w_rows = w_all.shape[1:]
    pieces = [(0, w_columns, False)]
    if w_columns % 16 == 0:
        cut = w_columns // 40 * 16
        pieces = [(0, cut, False), (cut, cut, False), (2 * cut, w_columns - 2 * cut, True)]
    plain = [p for p in range(len(pieces)) if not pieces[p][2]]
    turned = [p for p in range(len(pieces)) if pieces[p][2]]
    kv = gather_plan(kv_all, (kzs, kzr, kys, kyr, kcs, kcr), z_count, z, y, c)
    w = line_plan(w_all, pieces, (wzs, wzr, wys, wyr, wcs, wcr), z_count, z, y, c)
    kv[0]()
    kv[1](0)
    loads[2].wait()
    for p in turned + plain[:1]:
        w[1](p)
    for p in plain + turned:
        w[0](p)
    loads[3].wait()
    for i in range(HEADS // 2):
        pair = rotated(q_raw[:, i * 2 * HD:(i + 1) * 2 * HD]) * jnp.bfloat16(HD ** -0.5)
        g, inside = (2 * i) // group_size, (2 * i) % group_size
        q_rot[g, inside * rows:(inside + 1) * rows, :] = pair[:, :HD]
        q_rot[g, (inside + 1) * rows:(inside + 2) * rows, :] = pair[:, HD:]
    key_row = lax.broadcasted_iota(jnp.int32, (1, key_count), 1)
    span_of_key = jnp.zeros((1, key_count), jnp.int32)
    for i in range(span_ref.shape[1]):
        span_of_key = jnp.where(key_row // HALF == i, span_ref[0, i], span_of_key)
    key_at = span_of_key * HALF + key_row % HALF
    query_at = spot(lax.broadcasted_iota(jnp.int32, (rows, 1), 0))
    bias[...] = jnp.where(key_at <= query_at, 0.0, masked_score)

    for load in loads[10:]:
        load.wait()
    chosen = routing_ref[...]
    expert_row = lax.broadcasted_iota(jnp.int32, (EXPERTS, rows), 0)
    picks = [chosen[j:j + 1, :] == expert_row for j in range(TOPK)]
    named = sum(p.astype(jnp.float32) for p in picks)
    earlier = lax.broadcasted_iota(jnp.int32, (rows, rows), 0) < lax.broadcasted_iota(
        jnp.int32, (rows, rows), 1
    )
    before = jnp.dot(named, earlier.astype(jnp.float32), preferred_element_type=jnp.float32)
    slots = [
        jnp.sum(jnp.where(p, before, 0.0), axis=0, keepdims=True).astype(jnp.int32) for p in picks
    ]

    column = lax.broadcasted_iota(jnp.int32, (1, 2 * rows), 1)
    wrap = column // rows
    chosen_twice = jnp.concatenate([chosen, chosen], axis=1)
    slot_twice = [jnp.concatenate([slots[j], slots[j]], axis=1) for j in range(TOPK)]
    place = lax.broadcasted_iota(jnp.int32, (EXPERTS * 2 * CAP, 2 * rows), 0)
    dispatch[...] = sum(
        (place == chosen_twice[j:j + 1, :] * (2 * CAP) + wrap * CAP + slot_twice[j]).astype(jnp.float32)
        for j in range(TOPK)
    ).astype(jnp.bfloat16)

    for d in range(1, z_count):
        kv[1](d)
        if d == 1:
            for p in turned:
                w[3](-1, p)
    for load in loads[6:9]:
        load.start()
    for p in plain[1:]:
        w[1](p)
    for p in plain:
        w[2](0, p)
    for d in range(z_count):
        kv[2](d)
    w[3](-1, plain[0])
    kv[3]()
    steps = [functools.partial(w[3], -1, p) for p in plain[1:]]
    steps += [functools.partial(w[2], 0, p) for p in turned]
    for k in range(1, z_count - 1):
        for p in plain:
            steps += [functools.partial(w[2], k, p), functools.partial(w[3], k - 1, p)]
        steps += [functools.partial(w[2], k, p) for p in turned]
    closing = [functools.partial(w[3], z_count - 2, p) for p in plain]

    chunk = 4

    def send_rows(g):
        return [
            remote(
                rows_all.at[g, f_me], rows_all.at[g, f_me], as_.at[g, d], ar.at[g, d],
                fsdp=lax.rem(f_me + d, fsdp_count),
            )
            for d in range(1, fsdp_count)
        ]

    row_copies = [send_rows(g) for g in range(KVH)]
    turns = KVH * group_size // chunk
    share = max(1, len(steps) // turns)
    for g in range(KVH):
        keys = kv_all[:, :, g * HD:(g + 1) * HD].reshape(key_count, HD)
        vals = kv_all[:, :, (KVH + g) * HD:(KVH + g + 1) * HD].reshape(key_count, HD)
        parts = []
        for part in range(group_size // chunk):
            q = q_rot[g, part * chunk * rows:(part + 1) * chunk * rows, :]
            s = lax.dot_general(q, keys, (((1,), (1,)), ((), ())), preferred_element_type=jnp.float32)
            weights, totals = [], []
            for i in range(chunk):
                sink = sink_ref[0, g * group_size + part * chunk + i]
                one = s[i * rows:(i + 1) * rows, :] + bias[...]
                top = jnp.maximum(jnp.max(one, axis=1, keepdims=True), sink)
                p = jnp.exp(one - top)
                totals.append(jnp.sum(p, axis=1, keepdims=True) + jnp.exp(sink - top))
                weights.append(p.astype(jnp.bfloat16))
            o = jnp.dot(jnp.concatenate(weights, axis=0), vals, preferred_element_type=jnp.float32)
            for i in range(chunk):
                parts.append((o[i * rows:(i + 1) * rows, :] / totals[i]).astype(jnp.bfloat16))
            if part == group_size // chunk - 1:
                rows_all[g, pl.ds(f_me, 1)] = jnp.concatenate(parts, axis=1)[None]
                for copy in row_copies[g]:
                    copy.start()
            for step in steps[:share]:
                step()
            steps = steps[share:]
    for step in steps:
        step()
    loads[4].wait()
    loads[5].wait()

    width = group_size * HD
    count = width // w_rows
    pair = max(1, 256 // w_rows)
    upward = list(range(KVH))
    downward = [*range(KVH - 2, 0, -1), KVH - 1, 0]
    total = None
    for i in range(KVH):
        g = jnp.where(z < z_count // 2, upward[i], downward[i])
        if i == KVH - 1:
            for step in closing:
                step()
        for zz in range(z_count // KVH):
            w[4](g * (z_count // KVH) + zz)
        for copy in send_rows(g):
            copy.wait_recv()
        for first in range(0, count, pair):
            block = jnp.concatenate([w_all[g * count + first + i] for i in range(pair)], axis=1)
            term = lax.dot_general(
                rows_all[g, :, :, first * w_rows:(first + pair) * w_rows].reshape(
                    fsdp_count * rows, pair * w_rows
                ),
                block, (((1,), (1,)), ((), ())), preferred_element_type=jnp.float32,
            )
            total = term if total is None else total + term
    proj[...] = total.astype(jnp.bfloat16).reshape(proj.shape)
    backs = []
    for d in range(1, fsdp_count):
        peer = lax.rem(f_me + d, fsdp_count)
        backs.append(remote(proj.at[peer], got.at[f_me], ps.at[d], pr.at[d], fsdp=peer))
    for copy in backs:
        copy.start()

    shares, thin = x_out.shape[0], x_out.shape[3]
    widths = [w_columns, D - w_columns] if shares == 2 else [D]

    def share_of(t, wide):
        if shares == 1:
            return wide
        return jnp.where(f_me == t, wide[:, :w_columns], wide[:, w_columns:])

    def rows_of(t, weight):
        if shares == 1:
            return weight[...]
        return weight[pl.ds((f_me if t == 0 else 1 - f_me) * w_columns, w_columns), :]

    sends, returns = [{} for _ in range(shares)], {}
    for r, rel in enumerate(relative[1:], 1):
        to, source = peer_of(*rel), peer_of(*rel, sign=-1)
        for t in range(shares):
            sends[t][r] = remote(
                x_out.at[t, to // copies], arrived.at[t, r], xs.at[t, r], xr.at[t, r], seq=to
            )
        returns[r] = remote(back.at[r], returned.at[me], bs.at[r], br.at[r], seq=source)

    def send_share(t, scaled, tail):
        full = jnp.concatenate([scaled, tail], axis=1).astype(jnp.bfloat16)
        both = jnp.concatenate([full[:, :thin], full[:, thin:]], axis=0)
        buffer = jnp.dot(dispatch[...], both, preferred_element_type=jnp.float32).astype(jnp.bfloat16)
        for e in range(EXPERTS):
            x_out[t, e] = buffer[e * 2 * CAP:(e + 1) * 2 * CAP, :]
        for copy in sends[t].values():
            copy.start()

    gain = gain_ref[...][None, :].astype(jnp.float32)
    if shares == 2:
        local = share_of(0, res[...].astype(jnp.float32)) + proj[f_me].astype(jnp.float32)
        send_share(0, local * share_of(0, gain), jnp.zeros((rows, 2 * thin - w_columns), jnp.float32))
    got[pl.ds(f_me, 1)] = proj[pl.ds(f_me, 1)]
    kv[4]()
    w[5]()
    for g in range(KVH):
        for copy in row_copies[g]:
            copy.wait_send()
    for copy in backs:
        copy.wait_recv()
    for f in range(fsdp_count):
        out_ref[0, :, f * w_columns:(f + 1) * w_columns] = got[f]
    for copy in backs:
        copy.wait_send()

    stream = res[...].astype(jnp.float32) + out_ref[0].astype(jnp.float32)
    scale = lax.rsqrt(jnp.mean(stream * stream, axis=-1, keepdims=True) + norm_eps)
    scale_high = scale.astype(jnp.bfloat16).astype(jnp.float32)
    tail_lane = lax.broadcasted_iota(jnp.int32, (rows, 2 * thin - widths[-1]), 1)
    tail = jnp.where(tail_lane == 0, scale_high, jnp.where(tail_lane == 1, scale - scale_high, 0.0))
    send_share(shares - 1, share_of(1, stream * gain), tail)
    normed = (stream * scale * gain).astype(jnp.bfloat16)

    fold = back.shape[2]
    spare = 2 * fold - D

    def folded(wide):
        right = jnp.concatenate([wide[:, fold:], jnp.zeros((wide.shape[0], spare), wide.dtype)], axis=1)
        return wide[:, :fold], right

    logits = lax.dot_general(
        router[...], normed, (((1,), (1,)), ((), ())), preferred_element_type=jnp.float32
    )
    told = [jnp.sum(jnp.where(p, logits, 0.0), axis=0, keepdims=True) for p in picks]
    gates = [1.0 / sum(jnp.exp(t - told[j]) for t in told) for j in range(TOPK)]
    slot_row = lax.broadcasted_iota(jnp.int32, (seq_count * 2 * CAP, 2 * rows), 0)
    within = slot_row % (2 * CAP)
    mixing = sum(
        jnp.where(
            (slot_row // (2 * CAP * copies) == chosen_twice[j:j + 1, :])
            & (within == wrap * CAP + slot_twice[j]),
            jnp.concatenate([gates[j], gates[j]], axis=1),
            0.0,
        )
        for j in range(TOPK)
    )
    coarse = mixing.astype(jnp.bfloat16).astype(jnp.float32)
    mix[...] = jnp.concatenate([coarse, mixing - coarse], axis=1).T.astype(jnp.bfloat16)

    for load in loads[6:9]:
        load.wait()
    near = len(relative) // 2
    chunks = [range(near), range(near, near + near // 2), range(near + near // 2, 2 * near)]
    for chunk in chunks:
        g = u = 0.0
        count = len(chunk) * CAP
        for t in range(shares):
            for i, r in enumerate(chunk):
                if r > 0:
                    sends[t][r].wait_recv()
                    block = arrived[t, r]
                else:
                    block = x_out[t, me // copies]
                stacked[t, i * CAP:(i + 1) * CAP, :thin] = block[:CAP, :]
                stacked[t, i * CAP:(i + 1) * CAP, thin:] = block[CAP:, :]
            x = stacked[t, :count, :widths[t]]
            g = g + jnp.dot(x, rows_of(t, gate), preferred_element_type=jnp.float32)
            u = u + jnp.dot(x, rows_of(t, up), preferred_element_type=jnp.float32)
        scales = stacked[shares - 1, :count, widths[-1]:widths[-1] + 2].astype(jnp.float32)
        scales = scales[:, :1] + scales[:, 1:]
        g, u = g * scales, u * scales
        hidden = (g * jax.nn.sigmoid(1.702 * g) * (u + 1.0)).astype(jnp.bfloat16)
        part = jnp.dot(hidden, down[...], preferred_element_type=jnp.float32).astype(jnp.bfloat16)
        left, right = folded(part)
        for i, r in enumerate(chunk):
            target = back.at[r] if r > 0 else returned.at[me]
            target[:CAP] = left[i * CAP:(i + 1) * CAP, :]
            target[CAP:] = right[i * CAP:(i + 1) * CAP, :]
            if r > 0:
                returns[r].start()
    for share in sends:
        for copy in share.values():
            copy.wait_send()
    for copy in returns.values():
        copy.wait_recv()
    parts = jnp.dot(
        mix[...], returned[...].reshape(seq_count * 2 * CAP, fold), preferred_element_type=jnp.float32
    )
    mixed = [parts[h * rows:(h + 1) * rows, :] + parts[(2 + h) * rows:(3 + h) * rows, :] for h in range(2)]
    stream = res[...].astype(jnp.float32) + out_ref[0].astype(jnp.float32)
    out_ref[1, :, :fold] = (stream[:, :fold] + mixed[0]).astype(jnp.bfloat16)
    out_ref[1, :, fold:] = (stream[:, fold:] + mixed[1][:, :D - fold]).astype(jnp.bfloat16)
    for copy in returns.values():
        copy.wait_send()


def on_device(
    residual,
    queries,
    key_rows,
    values,
    attention_sinks,
    out_weight,
    norm_gain,
    router_weight,
    gate_weight,
    up_weight,
    down_weight,
    routing,
    span_order,
):
    seq_count = lax.axis_size("seq")
    fsdp_count = lax.axis_size("fsdp")
    z_count = seq_count // 4
    rows = residual.shape[1]
    dma = pltpu.SemaphoreType.DMA
    vmem = pl.BlockSpec(memory_space=pltpu.VMEM)
    hbm = pl.BlockSpec(memory_space=pltpu.HBM)

    def held(*shape):
        return pltpu.VMEM(shape, jnp.bfloat16)

    kv_width = 2 * KVH * HD
    fold = -(-D // 256) * 128
    w_rows, columns = out_weight.shape
    shares = 2 if fsdp_count == 2 and columns % 16 == 0 else 1
    thin = -(-((columns if shares == 2 else D) + 2) // 256) * 128
    both = pl.pallas_call(
        functools.partial(layer_kernel, seq_count, fsdp_count),
        out_shape=jax.ShapeDtypeStruct((2, rows, D), jnp.bfloat16),
        in_specs=[hbm] * 13,
        out_specs=vmem,
        scratch_shapes=[
            pltpu.SMEM((1, HEADS), jnp.float32),
            pltpu.SMEM((1, span_order.shape[0]), jnp.int32),
            held(D),
            pltpu.VMEM((TOPK, rows), jnp.int32),
            held(rows, D),
            held(rows, HEADS * HD),
            held(rows, KVH * HD),
            held(rows, KVH * HD),
            held(*router_weight.shape[::-1]),
            held(*gate_weight.shape),
            held(*up_weight.shape),
            held(*down_weight.shape),
            held(seq_count, rows, kv_width),
            held(seq_count, columns, w_rows),
            held(KVH, HEADS // KVH * rows, HD),
            pltpu.VMEM((rows, seq_count * rows), jnp.float32),
            held(KVH, fsdp_count, rows, HEADS // KVH * HD),
            held(fsdp_count, rows, columns),
            held(fsdp_count, rows, columns),
            held(shares, EXPERTS, 2 * CAP, thin),
            held(shares, seq_count, 2 * CAP, thin),
            held(shares, seq_count // 2 * CAP, 2 * thin),
            held(seq_count, 2 * CAP, fold),
            held(seq_count, 2 * CAP, fold),
            held(4 * rows, seq_count * 2 * CAP),
            held(EXPERTS * 2 * CAP, 2 * rows),
            dma((13,)),
        ]
        + [dma((z_count,))] * 4
        + [dma((2, z_count))] * 2
        + [dma((2, 2, z_count, 3)), dma((2, z_count, 3)), dma((z_count, 3)), dma((z_count, 3))]
        + [dma((2, z_count, 3))] * 2
        + [dma((KVH, fsdp_count)), dma((KVH, fsdp_count)), dma((fsdp_count,)), dma((fsdp_count,))]
        + [dma((shares, seq_count))] * 2
        + [dma((seq_count,))] * 2,
        compiler_params=pltpu.CompilerParams(
            collective_id=0, has_side_effects=True, vmem_limit_bytes=60 * 1024 * 1024
        ),
    )(
        attention_sinks[None, :],
        span_order[None, :],
        norm_gain,
        routing[0].T,
        residual[0],
        queries[0],
        key_rows[0],
        values[0],
        out_weight.T,
        router_weight.T,
        gate_weight,
        up_weight,
        down_weight,
    )
    return (both[0][None], both[1][None])


def solution(mesh):
    in_specs = (
        P("fsdp", "seq", None),
        P("fsdp", "seq", None),
        P("fsdp", "seq", None),
        P("fsdp", "seq", None),
        P(),
        P("seq", "fsdp"),
        P(),
        P(),
        P(None, "seq"),
        P(None, "seq"),
        P("seq", None),
        P("fsdp", "seq", None),
        P(),
    )
    out_specs = (P("fsdp", "seq", None), P("fsdp", "seq", None))
    return jax.shard_map(
        on_device, mesh=mesh, in_specs=in_specs, out_specs=out_specs, check_vma=False
    )
```

```python
import functools

import jax
import jax.numpy as jnp
from jax import lax
from jax.experimental import pallas as pl
from jax.experimental.pallas import tpu as pltpu
from jax.sharding import PartitionSpec as P

D = 1440
HEADS = 32
KVH = 4
HD = 64
EXPERTS = 16
TOPK = 2
TOK_DEV = 64
HALF = 32
CAP = 12


rope_base = 150000.0
norm_eps = 1e-05
masked_score = -1e30


MESH = pl.DeviceIdType.MESH


def remote(source, target, send_sem, recv_sem, **where):
    return pltpu.make_async_remote_copy(
        src_ref=source,
        dst_ref=target,
        send_sem=send_sem,
        recv_sem=recv_sem,
        device_id=where,
        device_id_type=MESH,
    )


KV_SENT, KV_BESIDE, W_OVER, W_TURNED, W_BESIDE, ROWS_SENT, X_SENT, BACK_SENT, BACK_HERE = range(9)


def settle(as_large, sem):
    pltpu.make_async_copy(as_large, as_large, sem).wait()


def slot(z, y, c):
    return (z * 2 + y) * 2 + c


def plane(far, j, z, z_count, sign=1):
    reach = z_count // 2
    base, inner = z // reach, lax.rem(z, reach)
    step = lax.rem(inner + j, reach) if sign > 0 else lax.rem(inner + reach - j, reach)
    return (1 - base if far else base) * reach + step


def gather_plan(slots, sems, z_count, z, y, c):
    z_recv, y_recv, once = sems
    reach = z_count // 2
    order = [(0, 0)] + [(1, j) for j in range(reach)] + [(0, j) for j in range(1, reach)]

    def z_of(d):
        return plane(*order[d], z, z_count, sign=-1)

    own = slots.at[slot(z, y, c)]
    to_z = [
        remote(own, own, once.at[KV_SENT], z_recv.at[d], seq=slot(plane(*order[d], z, z_count), y, c))
        for d in range(1, z_count)
    ]

    def to_y(d):
        block = slots.at[slot(z_of(d), y, c)]
        return remote(block, block, once.at[KV_SENT], y_recv.at[d], seq=slot(z, 1 - y, c))

    def to_c(side, d):
        block = slots.at[slot(z_of(d), y if side == 0 else 1 - y, c)]
        return remote(block, block, once.at[KV_SENT], once.at[KV_BESIDE], seq=slot(z, y, 1 - c))

    ys = [to_y(d) for d in range(z_count)]
    cs = [[to_c(side, d) for d in range(z_count)] for side in range(2)]

    def start_z():
        for copy in to_z:
            copy.start()

    def relay(d):
        if d > 0:
            to_z[d - 1].wait_recv()
        ys[d].start()
        cs[0][d].start()

    def relay_across(d):
        ys[d].wait_recv()
        cs[1][d].start()

    def finish():
        settle(slots.at[pl.ds(0, 2 * z_count)], once.at[KV_BESIDE])

    def drain():
        settle(slots.at[pl.ds(0, 4 * z_count - 1)], once.at[KV_SENT])

    return start_z, relay, relay_across, finish, drain


def line_plan(slots, pieces, sems, z_count, z, y, c):
    z_send, z_recv, y_recv, c_recv, once = sems
    last = z_count - 1

    def block(side, zz, p):
        start, size, _ = pieces[p]
        return slots.at[slot(zz, 1 - y if side else y, c), pl.ds(start, size)]

    def along(way, side, zz, p):
        part = block(side, zz, p)
        lane = len(pieces) if side else p
        sent = jnp.where((zz == z) & (way == 1), z_count, zz)
        return remote(part, part, z_send.at[sent, lane], z_recv.at[zz, lane], seq=slot(z + 1 - 2 * way, y, c))

    def over(zz, p):
        part = block(0, zz, p)
        sent = once.at[W_TURNED if pieces[p][2] else W_OVER]
        return remote(part, part, sent, y_recv.at[zz, p], seq=slot(z, 1 - y, c))

    def beside(side, zz, p):
        part = block(side, zz, p)
        return remote(part, part, once.at[W_BESIDE], c_recv.at[zz], seq=slot(z, y, 1 - c))

    def sides(p):
        return range(2) if pieces[p][2] else range(1)

    def onward(way, side, zz, p):
        @pl.when(z < last if way == 0 else z > 0)
        def _():
            along(way, side, zz, p).start()

    def start(p):
        onward(0, 0, z, p)
        onward(1, 0, z, p)
        beside(0, z, p).start()

    def cross(p):
        over(z, p).start()

    def each(k, act):
        for way in range(2):
            zz = z - 1 - k if way == 0 else z + 1 + k

            @pl.when(zz >= 0 if way == 0 else zz <= last)
            def _(way=way, zz=zz):
                act(way, zz)

    def relay(k, p):
        def act(way, zz):
            for side in sides(p):
                along(way, side, zz, p).wait_recv()
                onward(way, side, zz, p)
                beside(side, zz, p).start()
            if not pieces[p][2]:
                over(zz, p).start()

        each(k, act)

    def across(k, p):
        def act(way, zz):
            over(zz, p).wait_recv()
            beside(1, zz, p).start()
            if pieces[p][2]:
                onward(0, 1, zz, p)
                onward(1, 1, zz, p)

        if k < 0:
            act(0, z)
        else:
            each(k, act)

    def ready(zz):
        settle(slots.at[pl.ds(0, 2)], c_recv.at[zz])

    def drain():
        for p in range(len(pieces)):
            for zz in range(z_count):
                for side in sides(p):
                    @pl.when((z >= zz) & (z < last))
                    def _():
                        along(0, side, zz, p).wait_send()

                    @pl.when((z <= zz) & (z > 0))
                    def _():
                        along(1, side, zz, p).wait_send()

            if pieces[p][2]:
                over(z, p).wait_send()
        straight = sum(size for _, size, turned in pieces if not turned)
        settle(slots.at[pl.ds(0, z_count), pl.ds(0, straight)], once.at[W_OVER])
        settle(slots.at[pl.ds(0, 2 * z_count)], once.at[W_BESIDE])

    return start, cross, relay, across, ready, drain


def layer_kernel(
    seq_count, fsdp_count,
    sink_hbm, span_hbm, gain_hbm, routing_hbm, res_hbm, q_hbm, k_hbm, v_hbm, w_hbm, router_hbm, gate_hbm, up_hbm, down_hbm,
    out_ref,
    sink_ref, span_ref, gain_ref, routing_ref, res, q_raw, k_raw, v_raw, router, gate, up, down,
    kv_all, w_all, q_rot, bias, rows_all, proj, got,
    x_out, arrived, stacked, begun, back, returned, mix, dispatch,
    load_sems,
    kzr, kyr, wzs, wzr, wyr, wcr, ar, ps, pr, xr, once,
):
    me = lax.axis_index("seq")
    f_me = lax.axis_index("fsdp")
    sources = (
        k_hbm, v_hbm, w_hbm, q_hbm, res_hbm, router_hbm, gate_hbm, up_hbm, down_hbm,
        span_hbm, sink_hbm, routing_hbm, gain_hbm,
    )
    targets = (
        k_raw, v_raw, w_all.at[me], q_raw, res, router, gate, up, down, span_ref, sink_ref, routing_ref, gain_ref,
    )
    loads = [
        pltpu.make_async_copy(a, b, load_sems.at[i]) for i, (a, b) in enumerate(zip(sources, targets))
    ]
    for load in loads[9:] + loads[:6]:
        load.start()

    z_count = seq_count // 4
    z, y, c = me // 4, lax.rem(me // 2, 2), lax.rem(me, 2)
    reach = z_count // 2

    def peer_of(far, j, side, cc, sign=1):
        zz = plane(far, j, z, z_count, sign)
        return (zz * 2 + (1 - y if side else y)) * 2 + (1 - c if cc else c)

    relative = [
        (far, j, side, cc) for far in range(2) for j in range(reach) for side in range(2) for cc in range(2)
    ]
    peers = [{"seq": peer_of(*r)} for r in relative[1:]]
    peers += [{"fsdp": lax.rem(f_me + d, fsdp_count)} for d in range(1, fsdp_count)]
    barrier = pltpu.get_barrier_semaphore()
    for where in peers:
        pl.semaphore_signal(barrier, inc=1, device_id=where, device_id_type=MESH)

    rows, key_count = bias.shape
    group_size = HEADS // KVH
    copies = seq_count // EXPERTS

    loads[9].wait()

    def spot(row):
        return jnp.where(row < HALF, span_ref[0, 2 * me], span_ref[0, 2 * me + 1]) * HALF + row % HALF

    lane = lax.broadcasted_iota(jnp.int32, (rows, 2 * HD), 1)
    place = spot(lax.broadcasted_iota(jnp.int32, (rows, 2 * HD), 0)).astype(jnp.float32)
    half = HD // 2
    frequency = jnp.exp(-jnp.log(rope_base) * (lane % half).astype(jnp.float32) / half)
    angles = place * frequency
    low = (lane % HD) < half
    cosine = jnp.cos(angles)
    sine = jnp.where(low, -jnp.sin(angles), jnp.sin(angles))

    def rotated(pair):
        x = pair.astype(jnp.float32)
        swapped = jnp.where(low, pltpu.roll(x, 2 * HD - half, 1), pltpu.roll(x, half, 1))
        return (x * cosine + swapped * sine).astype(jnp.bfloat16)

    loads[0].wait()
    loads[1].wait()
    keys = [rotated(k_raw[:, i * 2 * HD:(i + 1) * 2 * HD]) for i in range(KVH // 2)]
    kv_all[pl.ds(me, 1)] = jnp.concatenate(keys + [v_raw[...]], axis=1)[None]

    pl.semaphore_wait(barrier, len(peers))

    w_columns, w_rows = w_all.shape[1:]
    pieces = [(0, w_columns, False)]
    if w_columns % 16 == 0:
        cut = w_columns // 40 * 16
        pieces = [(0, cut, False), (cut, cut, False), (2 * cut, w_columns - 2 * cut, True)]
    plain = [p for p in range(len(pieces)) if not pieces[p][2]]
    turned = [p for p in range(len(pieces)) if pieces[p][2]]
    kv = gather_plan(kv_all, (kzr, kyr, once), z_count, z, y, c)
    w = line_plan(w_all, pieces, (wzs, wzr, wyr, wcr, once), z_count, z, y, c)
    kv[0]()
    kv[1](0)
    loads[2].wait()
    for p in turned + plain[:1]:
        w[1](p)
    for p in plain + turned:
        w[0](p)
    loads[3].wait()
    for i in range(HEADS // 2):
        pair = rotated(q_raw[:, i * 2 * HD:(i + 1) * 2 * HD]) * jnp.bfloat16(HD ** -0.5)
        g, inside = (2 * i) // group_size, (2 * i) % group_size
        q_rot[g, inside * rows:(inside + 1) * rows, :] = pair[:, :HD]
        q_rot[g, (inside + 1) * rows:(inside + 2) * rows, :] = pair[:, HD:]
    key_row = lax.broadcasted_iota(jnp.int32, (1, key_count), 1)
    span_of_key = jnp.zeros((1, key_count), jnp.int32)
    for i in range(span_ref.shape[1]):
        span_of_key = jnp.where(key_row // HALF == i, span_ref[0, i], span_of_key)
    key_at = span_of_key * HALF + key_row % HALF
    query_at = spot(lax.broadcasted_iota(jnp.int32, (rows, 1), 0))
    bias[...] = jnp.where(key_at <= query_at, 0.0, masked_score)

    for load in loads[10:]:
        load.wait()
    chosen = routing_ref[...]
    expert_row = lax.broadcasted_iota(jnp.int32, (EXPERTS, rows), 0)
    picks = [chosen[j:j + 1, :] == expert_row for j in range(TOPK)]
    named = sum(p.astype(jnp.float32) for p in picks)
    earlier = lax.broadcasted_iota(jnp.int32, (rows, rows), 0) < lax.broadcasted_iota(
        jnp.int32, (rows, rows), 1
    )
    before = jnp.dot(named, earlier.astype(jnp.float32), preferred_element_type=jnp.float32)
    slots = [
        jnp.sum(jnp.where(p, before, 0.0), axis=0, keepdims=True).astype(jnp.int32) for p in picks
    ]

    column = lax.broadcasted_iota(jnp.int32, (1, 2 * rows), 1)
    wrap = column // rows
    chosen_twice = jnp.concatenate([chosen, chosen], axis=1)
    slot_twice = [jnp.concatenate([slots[j], slots[j]], axis=1) for j in range(TOPK)]
    place = lax.broadcasted_iota(jnp.int32, (EXPERTS * 2 * CAP, 2 * rows), 0)
    dispatch[...] = sum(
        (place == chosen_twice[j:j + 1, :] * (2 * CAP) + wrap * CAP + slot_twice[j]).astype(jnp.float32)
        for j in range(TOPK)
    ).astype(jnp.bfloat16)

    for d in range(1, z_count):
        kv[1](d)
        if d == 1:
            for p in turned:
                w[3](-1, p)
    for load in loads[6:9]:
        load.start()
    for p in plain[1:]:
        w[1](p)
    for p in plain:
        w[2](0, p)
    for d in range(z_count):
        kv[2](d)
    w[3](-1, plain[0])
    for p in turned:
        w[2](0, p)
    kv[3]()

    chunk = 4

    halves = group_size // chunk

    def send_rows(g, part):
        columns = rows_all.at[g, f_me, :, pl.ds(part * chunk * HD, chunk * HD)]
        return [
            remote(
                columns, columns, once.at[ROWS_SENT], ar.at[g, part, d - 1], fsdp=lax.rem(f_me + d, fsdp_count)
            )
            for d in range(1, fsdp_count)
        ]

    turns = KVH * group_size // chunk
    agenda = [[] for _ in range(turns)]

    def plan(turn, act, k, p):
        agenda[min(turn, turns - 1)].append(functools.partial(act, k, p))

    for p in plain[1:]:
        plan(0, w[3], -1, p)
    for k in range(1, z_count - 1):
        for i, p in enumerate(plain):
            if k == 1 and i == 0:
                w[2](k, p)
            else:
                plan(3 * (k - 1) + max(i - (k == 1), 0), w[2], k, p)
        for p in turned:
            plan(3 * k - 1, w[2], k, p)
        for i, p in enumerate(plain):
            plan(3 * k + 1 + i, w[3], k - 1, p)
    closing = [functools.partial(w[3], z_count - 2, p) for p in plain]
    for g in range(KVH):
        keys = kv_all[:, :, g * HD:(g + 1) * HD].reshape(key_count, HD)
        vals = kv_all[:, :, (KVH + g) * HD:(KVH + g + 1) * HD].reshape(key_count, HD)
        for part in range(halves):
            parts = []
            q = q_rot[g, part * chunk * rows:(part + 1) * chunk * rows, :]
            s = lax.dot_general(q, keys, (((1,), (1,)), ((), ())), preferred_element_type=jnp.float32)
            weights, totals = [], []
            for i in range(chunk):
                sink = sink_ref[0, g * group_size + part * chunk + i]
                one = s[i * rows:(i + 1) * rows, :] + bias[...]
                top = jnp.maximum(jnp.max(one, axis=1, keepdims=True), sink)
                p = jnp.exp(one - top)
                totals.append(jnp.sum(p, axis=1, keepdims=True) + jnp.exp(sink - top))
                weights.append(p.astype(jnp.bfloat16))
            o = jnp.dot(jnp.concatenate(weights, axis=0), vals, preferred_element_type=jnp.float32)
            for i in range(chunk):
                parts.append((o[i * rows:(i + 1) * rows, :] / totals[i]).astype(jnp.bfloat16))
            rows_all[g, f_me, :, part * chunk * HD:(part + 1) * chunk * HD] = jnp.concatenate(parts, axis=1)
            for copy in send_rows(g, part):
                copy.start()
            for step in agenda.pop(0):
                step()
    loads[4].wait()
    loads[5].wait()

    width = group_size * HD
    count = width // w_rows
    pair = max(1, 256 // w_rows)
    upward = list(range(KVH))
    downward = [*range(KVH - 2, 0, -1), KVH - 1, 0]
    total = None
    for i in range(KVH):
        g = jnp.where(z < z_count // 2, upward[i], downward[i])
        if i == 2 or (i == KVH - 1 and i < 2):
            for step in closing:
                step()
        for zz in range(z_count // KVH):
            w[4](g * (z_count // KVH) + zz)
        for part in range(halves):
            for copy in send_rows(g, part):
                copy.wait_recv()
        for first in range(0, count, pair):
            block = jnp.concatenate([w_all[g * count + first + i] for i in range(pair)], axis=1)
            term = lax.dot_general(
                rows_all[g, :, :, first * w_rows:(first + pair) * w_rows].reshape(
                    fsdp_count * rows, pair * w_rows
                ),
                block, (((1,), (1,)), ((), ())), preferred_element_type=jnp.float32,
            )
            total = term if total is None else total + term
    proj[...] = total.astype(jnp.bfloat16).reshape(proj.shape)
    backs = []
    for d in range(1, fsdp_count):
        peer = lax.rem(f_me + d, fsdp_count)
        backs.append(remote(proj.at[peer], got.at[f_me], ps.at[d], pr.at[d], fsdp=peer))
    for copy in backs:
        copy.start()

    shares, thin = x_out.shape[0], x_out.shape[3]
    widths = [w_columns, D - w_columns] if shares == 2 else [D]

    def share_of(t, wide):
        if shares == 1:
            return wide
        return jnp.where(f_me == t, wide[:, :w_columns], wide[:, w_columns:])

    def rows_of(t, weight):
        if shares == 1:
            return weight[...]
        return weight[pl.ds((f_me if t == 0 else 1 - f_me) * w_columns, w_columns), :]

    near = len(relative) // 2
    chunks = [range(near, near + near // 2), range(near + near // 2, 2 * near), range(near)]
    far_first = [r for chunk in chunks for r in chunk]
    chunk_of = {r: i for i, chunk in enumerate(chunks) for r in chunk}
    sends, returns = [{} for _ in range(shares)], {}
    for r, rel in enumerate(relative[1:], 1):
        to, source = peer_of(*rel), peer_of(*rel, sign=-1)
        for t in range(shares):
            sends[t][r] = remote(
                x_out.at[t, to // copies], arrived.at[t, r], once.at[X_SENT], xr.at[t, chunk_of[r]], seq=to
            )
        returns[r] = remote(back.at[r], returned.at[me], once.at[BACK_SENT], once.at[BACK_HERE], seq=source)

    late = [r for chunk in chunks for r in chunk if r > 0]
    early = late[:near // 2 + near // 4] if shares == 2 else []

    def send_share(t, scaled, tail):
        full = jnp.concatenate([scaled, tail], axis=1).astype(jnp.bfloat16)
        both = jnp.concatenate([full[:, :thin], full[:, thin:]], axis=0)
        buffer = jnp.dot(dispatch[...], both, preferred_element_type=jnp.float32).astype(jnp.bfloat16)
        for e in range(EXPERTS):
            x_out[t, e] = buffer[e * 2 * CAP:(e + 1) * 2 * CAP, :]
        if t < shares - 1:
            for r in early:
                sends[t][r].start()
            return
        for r in late:
            for other in range(shares - 1):
                if r not in early:
                    sends[other][r].start()
            sends[t][r].start()

    gain = gain_ref[...][None, :].astype(jnp.float32)
    if shares == 2:
        local = share_of(0, res[...].astype(jnp.float32)) + proj[f_me].astype(jnp.float32)
        send_share(0, local * share_of(0, gain), jnp.zeros((rows, 2 * thin - w_columns), jnp.float32))
    got[pl.ds(f_me, 1)] = proj[pl.ds(f_me, 1)]
    kv[4]()
    w[5]()
    if fsdp_count > 1:
        settle(rows_all.at[:, pl.ds(0, fsdp_count - 1)], once.at[ROWS_SENT])
    for copy in backs:
        copy.wait_recv()
    for f in range(fsdp_count):
        out_ref[0, :, f * w_columns:(f + 1) * w_columns] = got[f]
    for copy in backs:
        copy.wait_send()

    stream = res[...].astype(jnp.float32) + out_ref[0].astype(jnp.float32)
    scale = lax.rsqrt(jnp.mean(stream * stream, axis=-1, keepdims=True) + norm_eps)
    scale_high = scale.astype(jnp.bfloat16).astype(jnp.float32)
    tail_lane = lax.broadcasted_iota(jnp.int32, (rows, 2 * thin - widths[-1]), 1)
    tail = jnp.where(tail_lane == 0, scale_high, jnp.where(tail_lane == 1, scale - scale_high, 0.0))
    send_share(shares - 1, share_of(1, stream * gain), tail)
    normed = (stream * scale * gain).astype(jnp.bfloat16)

    fold = back.shape[2]
    spare = 2 * fold - D

    def folded(wide):
        right = jnp.concatenate([wide[:, fold:], jnp.zeros((wide.shape[0], spare), wide.dtype)], axis=1)
        return wide[:, :fold], right

    logits = lax.dot_general(
        router[...], normed, (((1,), (1,)), ((), ())), preferred_element_type=jnp.float32
    )
    told = [jnp.sum(jnp.where(p, logits, 0.0), axis=0, keepdims=True) for p in picks]
    gates = [1.0 / sum(jnp.exp(t - told[j]) for t in told) for j in range(TOPK)]
    slot_row = lax.broadcasted_iota(jnp.int32, (seq_count * 2 * CAP, 2 * rows), 0)
    within = slot_row % (2 * CAP)
    mixing = sum(
        jnp.where(
            (slot_row // (2 * CAP * copies) == chosen_twice[j:j + 1, :])
            & (within == wrap * CAP + slot_twice[j]),
            jnp.concatenate([gates[j], gates[j]], axis=1),
            0.0,
        )
        for j in range(TOPK)
    )
    coarse = mixing.astype(jnp.bfloat16).astype(jnp.float32)
    mix[...] = jnp.concatenate([coarse, mixing - coarse], axis=1).T.astype(jnp.bfloat16)

    for load in loads[6:9]:
        load.wait()

    def unpack(t, chunk, at):
        settle(arrived.at[t, pl.ds(0, sum(r > 0 for r in chunk))], xr.at[t, chunk_of[chunk[0]]])
        for r in chunk:
            block = arrived[t, r] if r > 0 else x_out[t, me // copies]
            stacked[t, at:at + CAP, :thin] = block[:CAP, :]
            stacked[t, at:at + CAP, thin:] = block[CAP:, :]
            at += CAP

    far_rows = near // 2 * CAP
    for t in range(shares - 1):
        unpack(t, chunks[0], 0)
        x = stacked[t, :far_rows, :widths[t]]
        begun[0] = jnp.dot(x, rows_of(t, gate), preferred_element_type=jnp.float32)
        begun[1] = jnp.dot(x, rows_of(t, up), preferred_element_type=jnp.float32)
    final = shares - 1
    for chunk in chunks:
        first, count = far_first.index(chunk[0]) * CAP, len(chunk) * CAP
        g = u = 0.0
        for t in range(shares):
            if t < final and first < far_rows:
                g, u = begun[0, first:first + count], begun[1, first:first + count]
                continue
            unpack(t, chunk, first)
            x = stacked[t, first:first + count, :widths[t]]
            g = g + jnp.dot(x, rows_of(t, gate), preferred_element_type=jnp.float32)
            u = u + jnp.dot(x, rows_of(t, up), preferred_element_type=jnp.float32)
        scales = stacked[final, first:first + count, widths[-1]:widths[-1] + 2].astype(jnp.float32)
        scales = scales[:, :1] + scales[:, 1:]
        g, u = g * scales, u * scales
        hidden = (g * jax.nn.sigmoid(1.702 * g) * (u + 1.0)).astype(jnp.bfloat16)
        part = jnp.dot(hidden, down[...], preferred_element_type=jnp.float32).astype(jnp.bfloat16)
        left, right = folded(part)
        for i, r in enumerate(chunk):
            target = back.at[r] if r > 0 else returned.at[me]
            target[:CAP] = left[i * CAP:(i + 1) * CAP, :]
            target[CAP:] = right[i * CAP:(i + 1) * CAP, :]
            if r > 0:
                returns[r].start()
    settle(arrived.at[:, pl.ds(0, seq_count - 1)], once.at[X_SENT])
    settle(returned.at[pl.ds(0, seq_count - 1)], once.at[BACK_HERE])
    parts = jnp.dot(
        mix[...], returned[...].reshape(seq_count * 2 * CAP, fold), preferred_element_type=jnp.float32
    )
    mixed = [parts[h * rows:(h + 1) * rows, :] + parts[(2 + h) * rows:(3 + h) * rows, :] for h in range(2)]
    stream = res[...].astype(jnp.float32) + out_ref[0].astype(jnp.float32)
    out_ref[1, :, :fold] = (stream[:, :fold] + mixed[0]).astype(jnp.bfloat16)
    out_ref[1, :, fold:] = (stream[:, fold:] + mixed[1][:, :D - fold]).astype(jnp.bfloat16)
    settle(returned.at[pl.ds(0, seq_count - 1)], once.at[BACK_SENT])


def on_device(
    residual,
    queries,
    key_rows,
    values,
    attention_sinks,
    out_weight,
    norm_gain,
    router_weight,
    gate_weight,
    up_weight,
    down_weight,
    routing,
    span_order,
):
    seq_count = lax.axis_size("seq")
    fsdp_count = lax.axis_size("fsdp")
    z_count = seq_count // 4
    rows = residual.shape[1]
    dma = pltpu.SemaphoreType.DMA
    vmem = pl.BlockSpec(memory_space=pltpu.VMEM)
    hbm = pl.BlockSpec(memory_space=pltpu.HBM)

    def held(*shape):
        return pltpu.VMEM(shape, jnp.bfloat16)

    kv_width = 2 * KVH * HD
    fold = -(-D // 256) * 128
    w_rows, columns = out_weight.shape
    shares = 2 if fsdp_count == 2 and columns % 16 == 0 else 1
    thin = -(-((columns if shares == 2 else D) + 2) // 256) * 128
    both = pl.pallas_call(
        functools.partial(layer_kernel, seq_count, fsdp_count),
        out_shape=jax.ShapeDtypeStruct((2, rows, D), jnp.bfloat16),
        in_specs=[hbm] * 13,
        out_specs=vmem,
        scratch_shapes=[
            pltpu.SMEM((1, HEADS), jnp.float32),
            pltpu.SMEM((1, span_order.shape[0]), jnp.int32),
            held(D),
            pltpu.VMEM((TOPK, rows), jnp.int32),
            held(rows, D),
            held(rows, HEADS * HD),
            held(rows, KVH * HD),
            held(rows, KVH * HD),
            held(*router_weight.shape[::-1]),
            held(*gate_weight.shape),
            held(*up_weight.shape),
            held(*down_weight.shape),
            held(seq_count, rows, kv_width),
            held(seq_count, columns, w_rows),
            held(KVH, HEADS // KVH * rows, HD),
            pltpu.VMEM((rows, seq_count * rows), jnp.float32),
            held(KVH, fsdp_count, rows, HEADS // KVH * HD),
            held(fsdp_count, rows, columns),
            held(fsdp_count, rows, columns),
            held(shares, EXPERTS, 2 * CAP, thin),
            held(shares, seq_count, 2 * CAP, thin),
            held(shares, seq_count * CAP, 2 * thin),
            pltpu.VMEM((2, seq_count // 4 * CAP, gate_weight.shape[1]), jnp.float32),
            held(seq_count, 2 * CAP, fold),
            held(seq_count, 2 * CAP, fold),
            held(4 * rows, seq_count * 2 * CAP),
            held(EXPERTS * 2 * CAP, 2 * rows),
            dma((13,)),
        ]
        + [dma((z_count,))] * 2
        + [dma((z_count + 1, 4)), dma((z_count, 4)), dma((z_count, 3)), dma((z_count,))]
        + [dma((KVH, 2, max(fsdp_count - 1, 1)))]
        + [dma((fsdp_count,))] * 2
        + [dma((shares, 3)), dma((9,))],
        compiler_params=pltpu.CompilerParams(
            collective_id=0, has_side_effects=True, vmem_limit_bytes=60 * 1024 * 1024
        ),
    )(
        attention_sinks[None, :],
        span_order[None, :],
        norm_gain,
        routing[0].T,
        residual[0],
        queries[0],
        key_rows[0],
        values[0],
        out_weight.T,
        router_weight.T,
        gate_weight,
        up_weight,
        down_weight,
    )
    return (both[0][None], both[1][None])


def solution(mesh):
    in_specs = (
        P("fsdp", "seq", None),
        P("fsdp", "seq", None),
        P("fsdp", "seq", None),
        P("fsdp", "seq", None),
        P(),
        P("seq", "fsdp"),
        P(),
        P(),
        P(None, "seq"),
        P(None, "seq"),
        P("seq", None),
        P("fsdp", "seq", None),
        P(),
    )
    out_specs = (P("fsdp", "seq", None), P("fsdp", "seq", None))
    return jax.shard_map(
        on_device, mesh=mesh, in_specs=in_specs, out_specs=out_specs, check_vma=False
    )
```

```python
import functools

import jax
import jax.numpy as jnp
from jax import lax
from jax.experimental import pallas as pl
from jax.experimental.pallas import tpu as pltpu
from jax.sharding import PartitionSpec as P

D = 1440
HEADS = 32
KVH = 4
HD = 64
EXPERTS = 16
TOPK = 2
TOK_DEV = 64
HALF = 32
CAP = 12


rope_base = 150000.0
norm_eps = 1e-05
masked_score = -1e30


MESH = pl.DeviceIdType.MESH
open_scope = []


def mark(name):
    while open_scope:
        open_scope.pop().__exit__(None, None, None)
    if name:
        open_scope.append(jax.named_scope(name))
        open_scope[-1].__enter__()


def remote(source, target, send_sem, recv_sem, **where):
    return pltpu.make_async_remote_copy(
        src_ref=source,
        dst_ref=target,
        send_sem=send_sem,
        recv_sem=recv_sem,
        device_id=where,
        device_id_type=MESH,
    )


KV_SENT, KV_BESIDE, W_OVER, W_TURNED, W_BESIDE, ROWS_SENT, X_SENT, BACK_SENT, BACK_HERE = range(9)


def settle(as_large, sem):
    pltpu.make_async_copy(as_large, as_large, sem).wait()


def slot(z, y, c):
    return (z * 2 + y) * 2 + c


def plane(far, j, z, z_count, sign=1):
    reach = z_count // 2
    base, inner = z // reach, lax.rem(z, reach)
    step = lax.rem(inner + j, reach) if sign > 0 else lax.rem(inner + reach - j, reach)
    return (1 - base if far else base) * reach + step


def gather_plan(slots, sems, z_count, z, y, c):
    z_recv, y_recv, once = sems
    reach = z_count // 2
    order = [(0, 0)] + [(1, j) for j in range(reach)] + [(0, j) for j in range(1, reach)]

    def z_of(d):
        return plane(*order[d], z, z_count, sign=-1)

    own = slots.at[slot(z, y, c)]
    to_z = [
        remote(own, own, once.at[KV_SENT], z_recv.at[d], seq=slot(plane(*order[d], z, z_count), y, c))
        for d in range(1, z_count)
    ]

    def to_y(d):
        block = slots.at[slot(z_of(d), y, c)]
        return remote(block, block, once.at[KV_SENT], y_recv.at[d], seq=slot(z, 1 - y, c))

    def to_c(side, d):
        block = slots.at[slot(z_of(d), y if side == 0 else 1 - y, c)]
        return remote(block, block, once.at[KV_SENT], once.at[KV_BESIDE], seq=slot(z, y, 1 - c))

    ys = [to_y(d) for d in range(z_count)]
    cs = [[to_c(side, d) for d in range(z_count)] for side in range(2)]

    def start_z():
        for copy in to_z:
            copy.start()

    def relay(d):
        if d > 0:
            to_z[d - 1].wait_recv()
        ys[d].start()
        cs[0][d].start()

    def relay_across(d):
        ys[d].wait_recv()
        cs[1][d].start()

    def finish():
        settle(slots.at[pl.ds(0, 2 * z_count)], once.at[KV_BESIDE])

    def drain():
        settle(slots.at[pl.ds(0, 4 * z_count - 1)], once.at[KV_SENT])

    return start_z, relay, relay_across, finish, drain


def line_plan(slots, pieces, sems, z_count, z, y, c):
    z_send, z_recv, y_recv, c_recv, once = sems
    last = z_count - 1

    def block(side, zz, p):
        start, size, _ = pieces[p]
        return slots.at[slot(zz, 1 - y if side else y, c), pl.ds(start, size)]

    def along(way, side, zz, p):
        part = block(side, zz, p)
        lane = len(pieces) if side else p
        sent = jnp.where((zz == z) & (way == 1), z_count, zz)
        return remote(part, part, z_send.at[sent, lane], z_recv.at[zz, lane], seq=slot(z + 1 - 2 * way, y, c))

    def over(zz, p):
        part = block(0, zz, p)
        sent = once.at[W_TURNED if pieces[p][2] else W_OVER]
        return remote(part, part, sent, y_recv.at[zz, p], seq=slot(z, 1 - y, c))

    def beside(side, zz, p):
        part = block(side, zz, p)
        return remote(part, part, once.at[W_BESIDE], c_recv.at[zz], seq=slot(z, y, 1 - c))

    def sides(p):
        return range(2) if pieces[p][2] else range(1)

    def onward(way, side, zz, p):
        @pl.when(z < last if way == 0 else z > 0)
        def _():
            along(way, side, zz, p).start()

    def start(p):
        onward(0, 0, z, p)
        onward(1, 0, z, p)
        beside(0, z, p).start()

    def cross(p):
        over(z, p).start()

    def each(k, act):
        for way in range(2):
            zz = z - 1 - k if way == 0 else z + 1 + k

            @pl.when(zz >= 0 if way == 0 else zz <= last)
            def _(way=way, zz=zz):
                act(way, zz)

    def relay(k, p):
        def act(way, zz):
            for side in sides(p):
                along(way, side, zz, p).wait_recv()
                onward(way, side, zz, p)
                beside(side, zz, p).start()
            if not pieces[p][2]:
                over(zz, p).start()

        each(k, act)

    def across(k, p):
        def act(way, zz):
            over(zz, p).wait_recv()
            beside(1, zz, p).start()
            if pieces[p][2]:
                onward(0, 1, zz, p)
                onward(1, 1, zz, p)

        if k < 0:
            act(0, z)
        else:
            each(k, act)

    def ready(zz):
        settle(slots.at[pl.ds(0, 2)], c_recv.at[zz])

    def drain():
        for p in range(len(pieces)):
            for zz in range(z_count):
                for side in sides(p):
                    @pl.when((z >= zz) & (z < last))
                    def _():
                        along(0, side, zz, p).wait_send()

                    @pl.when((z <= zz) & (z > 0))
                    def _():
                        along(1, side, zz, p).wait_send()

            if pieces[p][2]:
                over(z, p).wait_send()
        straight = sum(size for _, size, turned in pieces if not turned)
        settle(slots.at[pl.ds(0, z_count), pl.ds(0, straight)], once.at[W_OVER])
        settle(slots.at[pl.ds(0, 2 * z_count)], once.at[W_BESIDE])

    return start, cross, relay, across, ready, drain


def layer_kernel(
    seq_count, fsdp_count,
    sink_hbm, span_hbm, gain_hbm, routing_hbm, res_hbm, q_hbm, k_hbm, v_hbm, w_hbm, router_hbm, gate_hbm, up_hbm, down_hbm,
    out_ref,
    sink_ref, span_ref, gain_ref, routing_ref, res, q_raw, k_raw, v_raw, router, gate, up, down,
    kv_all, w_all, q_rot, bias, rows_all, proj, got,
    x_out, arrived, stacked, begun, back, returned, mix, dispatch,
    load_sems,
    kzr, kyr, wzs, wzr, wyr, wcr, ar, ps, pr, xr, once,
):
    me = lax.axis_index("seq")
    f_me = lax.axis_index("fsdp")
    sources = (
        k_hbm, v_hbm, w_hbm, q_hbm, res_hbm, router_hbm, gate_hbm, up_hbm, down_hbm,
        span_hbm, sink_hbm, routing_hbm, gain_hbm,
    )
    targets = (
        k_raw, v_raw, w_all.at[me], q_raw, res, router, gate, up, down, span_ref, sink_ref, routing_ref, gain_ref,
    )
    loads = [
        pltpu.make_async_copy(a, b, load_sems.at[i]) for i, (a, b) in enumerate(zip(sources, targets))
    ]
    for load in loads[9:] + loads[:6]:
        load.start()

    z_count = seq_count // 4
    z, y, c = me // 4, lax.rem(me // 2, 2), lax.rem(me, 2)
    reach = z_count // 2

    def peer_of(far, j, side, cc, sign=1):
        zz = plane(far, j, z, z_count, sign)
        return (zz * 2 + (1 - y if side else y)) * 2 + (1 - c if cc else c)

    relative = [
        (far, j, side, cc) for far in range(2) for j in range(reach) for side in range(2) for cc in range(2)
    ]
    peers = [{"seq": peer_of(*r)} for r in relative[1:]]
    peers += [{"fsdp": lax.rem(f_me + d, fsdp_count)} for d in range(1, fsdp_count)]
    barrier = pltpu.get_barrier_semaphore()
    for where in peers:
        pl.semaphore_signal(barrier, inc=1, device_id=where, device_id_type=MESH)

    rows, key_count = bias.shape
    group_size = HEADS // KVH
    copies = seq_count // EXPERTS

    mark("A0b")
    loads[9].wait()

    def spot(row):
        return jnp.where(row < HALF, span_ref[0, 2 * me], span_ref[0, 2 * me + 1]) * HALF + row % HALF

    lane = lax.broadcasted_iota(jnp.int32, (rows, 2 * HD), 1)
    place = spot(lax.broadcasted_iota(jnp.int32, (rows, 2 * HD), 0)).astype(jnp.float32)
    half = HD // 2
    frequency = jnp.exp(-jnp.log(rope_base) * (lane % half).astype(jnp.float32) / half)
    angles = place * frequency
    low = (lane % HD) < half
    cosine = jnp.cos(angles)
    sine = jnp.where(low, -jnp.sin(angles), jnp.sin(angles))

    def rotated(pair):
        x = pair.astype(jnp.float32)
        swapped = jnp.where(low, pltpu.roll(x, 2 * HD - half, 1), pltpu.roll(x, half, 1))
        return (x * cosine + swapped * sine).astype(jnp.bfloat16)

    mark("A1_krot")
    loads[0].wait()
    loads[1].wait()
    keys = [rotated(k_raw[:, i * 2 * HD:(i + 1) * 2 * HD]) for i in range(KVH // 2)]
    kv_all[pl.ds(me, 1)] = jnp.concatenate(keys + [v_raw[...]], axis=1)[None]

    mark("A2_greet")
    pl.semaphore_wait(barrier, len(peers))

    mark("A3_kvstart")
    w_columns, w_rows = w_all.shape[1:]
    pieces = [(0, w_columns, False)]
    if w_columns % 16 == 0:
        cut = w_columns // 40 * 16
        pieces = [(0, cut, False), (cut, cut, False), (2 * cut, w_columns - 2 * cut, True)]
    plain = [p for p in range(len(pieces)) if not pieces[p][2]]
    turned = [p for p in range(len(pieces)) if pieces[p][2]]
    kv = gather_plan(kv_all, (kzr, kyr, once), z_count, z, y, c)
    w = line_plan(w_all, pieces, (wzs, wzr, wyr, wcr, once), z_count, z, y, c)
    kv[0]()
    kv[1](0)
    mark("A4_wstart")
    loads[2].wait()
    for p in turned + plain[:1]:
        w[1](p)
    for p in plain + turned:
        w[0](p)
    mark("A5_qrot")
    loads[3].wait()
    for i in range(HEADS // 2):
        pair = rotated(q_raw[:, i * 2 * HD:(i + 1) * 2 * HD]) * jnp.bfloat16(HD ** -0.5)
        g, inside = (2 * i) // group_size, (2 * i) % group_size
        q_rot[g, inside * rows:(inside + 1) * rows, :] = pair[:, :HD]
        q_rot[g, (inside + 1) * rows:(inside + 2) * rows, :] = pair[:, HD:]
    mark("A6_bias")
    key_row = lax.broadcasted_iota(jnp.int32, (1, key_count), 1)
    span_of_key = jnp.zeros((1, key_count), jnp.int32)
    for i in range(span_ref.shape[1]):
        span_of_key = jnp.where(key_row // HALF == i, span_ref[0, i], span_of_key)
    key_at = span_of_key * HALF + key_row % HALF
    query_at = spot(lax.broadcasted_iota(jnp.int32, (rows, 1), 0))
    bias[...] = jnp.where(key_at <= query_at, 0.0, masked_score)

    for load in loads[10:]:
        load.wait()
    mark("A7_slots")
    chosen = routing_ref[...]
    expert_row = lax.broadcasted_iota(jnp.int32, (EXPERTS, rows), 0)
    picks = [chosen[j:j + 1, :] == expert_row for j in range(TOPK)]
    named = sum(p.astype(jnp.float32) for p in picks)
    earlier = lax.broadcasted_iota(jnp.int32, (rows, rows), 0) < lax.broadcasted_iota(
        jnp.int32, (rows, rows), 1
    )
    before = jnp.dot(named, earlier.astype(jnp.float32), preferred_element_type=jnp.float32)
    slots = [
        jnp.sum(jnp.where(p, before, 0.0), axis=0, keepdims=True).astype(jnp.int32) for p in picks
    ]

    column = lax.broadcasted_iota(jnp.int32, (1, 2 * rows), 1)
    wrap = column // rows
    chosen_twice = jnp.concatenate([chosen, chosen], axis=1)
    slot_twice = [jnp.concatenate([slots[j], slots[j]], axis=1) for j in range(TOPK)]
    place = lax.broadcasted_iota(jnp.int32, (EXPERTS * 2 * CAP, 2 * rows), 0)
    dispatch[...] = sum(
        (place == chosen_twice[j:j + 1, :] * (2 * CAP) + wrap * CAP + slot_twice[j]).astype(jnp.float32)
        for j in range(TOPK)
    ).astype(jnp.bfloat16)

    mark("B0_relayz")
    for d in range(1, z_count):
        kv[1](d)
        if d == 1:
            for p in turned:
                w[3](-1, p)
    for load in loads[6:9]:
        load.start()
    for p in plain[1:]:
        w[1](p)
    for p in plain:
        w[2](0, p)
    mark("B1b_relayy")
    for d in range(z_count):
        kv[2](d)
    w[3](-1, plain[0])
    for p in turned:
        w[2](0, p)
    mark("B3_kvfinish")
    kv[3]()

    mark("C0_attn")
    chunk = 4

    halves = group_size // chunk

    def send_rows(g, part):
        columns = rows_all.at[g, f_me, :, pl.ds(part * chunk * HD, chunk * HD)]
        return [
            remote(
                columns, columns, once.at[ROWS_SENT], ar.at[g, part, d - 1], fsdp=lax.rem(f_me + d, fsdp_count)
            )
            for d in range(1, fsdp_count)
        ]

    turns = KVH * group_size // chunk
    agenda = [[] for _ in range(turns)]

    def plan(turn, act, k, p):
        agenda[min(turn, turns - 1)].append(functools.partial(act, k, p))

    for p in plain[1:]:
        plan(0, w[3], -1, p)
    for k in range(1, z_count - 1):
        for i, p in enumerate(plain):
            if k == 1 and i == 0:
                w[2](k, p)
            else:
                plan(3 * (k - 1) + max(i - (k == 1), 0), w[2], k, p)
        for p in turned:
            plan(3 * k - 1, w[2], k, p)
        for i, p in enumerate(plain):
            plan(3 * k + 1 + i, w[3], k - 1, p)
    closing = [functools.partial(w[3], z_count - 2, p) for p in plain]
    for g in range(KVH):
        keys = kv_all[:, :, g * HD:(g + 1) * HD].reshape(key_count, HD)
        vals = kv_all[:, :, (KVH + g) * HD:(KVH + g + 1) * HD].reshape(key_count, HD)
        for part in range(halves):
            parts = []
            q = q_rot[g, part * chunk * rows:(part + 1) * chunk * rows, :]
            s = lax.dot_general(q, keys, (((1,), (1,)), ((), ())), preferred_element_type=jnp.float32)
            weights, totals = [], []
            for i in range(chunk):
                sink = sink_ref[0, g * group_size + part * chunk + i]
                one = s[i * rows:(i + 1) * rows, :] + bias[...]
                top = jnp.maximum(jnp.max(one, axis=1, keepdims=True), sink)
                p = jnp.exp(one - top)
                totals.append(jnp.sum(p, axis=1, keepdims=True) + jnp.exp(sink - top))
                weights.append(p.astype(jnp.bfloat16))
            o = jnp.dot(jnp.concatenate(weights, axis=0), vals, preferred_element_type=jnp.float32)
            for i in range(chunk):
                parts.append((o[i * rows:(i + 1) * rows, :] / totals[i]).astype(jnp.bfloat16))
            rows_all[g, f_me, :, part * chunk * HD:(part + 1) * chunk * HD] = jnp.concatenate(parts, axis=1)
            for copy in send_rows(g, part):
                copy.start()
            mark(f"C{g}{part}_steps")
            for step in agenda.pop(0):
                step()
            mark(f"C{g}{part}x_attn")
    loads[4].wait()
    loads[5].wait()

    mark("D0_proj")
    width = group_size * HD
    count = width // w_rows
    pair = max(1, 256 // w_rows)
    upward = list(range(KVH))
    downward = [*range(KVH - 2, 0, -1), KVH - 1, 0]
    total = None
    for i in range(KVH):
        g = jnp.where(z < z_count // 2, upward[i], downward[i])
        if i == 2 or (i == KVH - 1 and i < 2):
            for step in closing:
                step()
        mark(f"D0{i}_wwait")
        for zz in range(z_count // KVH):
            w[4](g * (z_count // KVH) + zz)
        for part in range(halves):
            for copy in send_rows(g, part):
                copy.wait_recv()
        for first in range(0, count, pair):
            block = jnp.concatenate([w_all[g * count + first + i] for i in range(pair)], axis=1)
            term = lax.dot_general(
                rows_all[g, :, :, first * w_rows:(first + pair) * w_rows].reshape(
                    fsdp_count * rows, pair * w_rows
                ),
                block, (((1,), (1,)), ((), ())), preferred_element_type=jnp.float32,
            )
            total = term if total is None else total + term
    proj[...] = total.astype(jnp.bfloat16).reshape(proj.shape)
    mark("D1_sendproj")
    backs = []
    for d in range(1, fsdp_count):
        peer = lax.rem(f_me + d, fsdp_count)
        backs.append(remote(proj.at[peer], got.at[f_me], ps.at[d], pr.at[d], fsdp=peer))
    for copy in backs:
        copy.start()

    mark("D1b_early")
    shares, thin = x_out.shape[0], x_out.shape[3]
    widths = [w_columns, D - w_columns] if shares == 2 else [D]

    def share_of(t, wide):
        if shares == 1:
            return wide
        return jnp.where(f_me == t, wide[:, :w_columns], wide[:, w_columns:])

    def rows_of(t, weight):
        if shares == 1:
            return weight[...]
        return weight[pl.ds((f_me if t == 0 else 1 - f_me) * w_columns, w_columns), :]

    near = len(relative) // 2
    chunks = [range(near, near + near // 2), range(near + near // 2, 2 * near), range(near)]
    far_first = [r for chunk in chunks for r in chunk]
    chunk_of = {r: i for i, chunk in enumerate(chunks) for r in chunk}
    sends, returns = [{} for _ in range(shares)], {}
    for r, rel in enumerate(relative[1:], 1):
        to, source = peer_of(*rel), peer_of(*rel, sign=-1)
        for t in range(shares):
            sends[t][r] = remote(
                x_out.at[t, to // copies], arrived.at[t, r], once.at[X_SENT], xr.at[t, chunk_of[r]], seq=to
            )
        returns[r] = remote(back.at[r], returned.at[me], once.at[BACK_SENT], once.at[BACK_HERE], seq=source)

    late = [r for chunk in chunks for r in chunk if r > 0]
    early = late[:near // 2 + near // 4] if shares == 2 else []

    def send_share(t, scaled, tail):
        full = jnp.concatenate([scaled, tail], axis=1).astype(jnp.bfloat16)
        both = jnp.concatenate([full[:, :thin], full[:, thin:]], axis=0)
        buffer = jnp.dot(dispatch[...], both, preferred_element_type=jnp.float32).astype(jnp.bfloat16)
        for e in range(EXPERTS):
            x_out[t, e] = buffer[e * 2 * CAP:(e + 1) * 2 * CAP, :]
        if t < shares - 1:
            for r in early:
                sends[t][r].start()
            return
        for r in late:
            for other in range(shares - 1):
                if r not in early:
                    sends[other][r].start()
            sends[t][r].start()

    gain = gain_ref[...][None, :].astype(jnp.float32)
    if shares == 2:
        local = share_of(0, res[...].astype(jnp.float32)) + proj[f_me].astype(jnp.float32)
        send_share(0, local * share_of(0, gain), jnp.zeros((rows, 2 * thin - w_columns), jnp.float32))
    got[pl.ds(f_me, 1)] = proj[pl.ds(f_me, 1)]
    mark("D2_drain")
    kv[4]()
    w[5]()
    if fsdp_count > 1:
        settle(rows_all.at[:, pl.ds(0, fsdp_count - 1)], once.at[ROWS_SENT])
    mark("D3_waitproj")
    for copy in backs:
        copy.wait_recv()
    mark("E0_norm")
    for f in range(fsdp_count):
        out_ref[0, :, f * w_columns:(f + 1) * w_columns] = got[f]
    for copy in backs:
        copy.wait_send()

    stream = res[...].astype(jnp.float32) + out_ref[0].astype(jnp.float32)
    mark("E1_late")
    scale = lax.rsqrt(jnp.mean(stream * stream, axis=-1, keepdims=True) + norm_eps)
    scale_high = scale.astype(jnp.bfloat16).astype(jnp.float32)
    tail_lane = lax.broadcasted_iota(jnp.int32, (rows, 2 * thin - widths[-1]), 1)
    tail = jnp.where(tail_lane == 0, scale_high, jnp.where(tail_lane == 1, scale - scale_high, 0.0))
    send_share(shares - 1, share_of(1, stream * gain), tail)
    normed = (stream * scale * gain).astype(jnp.bfloat16)

    fold = back.shape[2]
    spare = 2 * fold - D

    def folded(wide):
        right = jnp.concatenate([wide[:, fold:], jnp.zeros((wide.shape[0], spare), wide.dtype)], axis=1)
        return wide[:, :fold], right

    mark("E2_gates")
    logits = lax.dot_general(
        router[...], normed, (((1,), (1,)), ((), ())), preferred_element_type=jnp.float32
    )
    told = [jnp.sum(jnp.where(p, logits, 0.0), axis=0, keepdims=True) for p in picks]
    gates = [1.0 / sum(jnp.exp(t - told[j]) for t in told) for j in range(TOPK)]
    slot_row = lax.broadcasted_iota(jnp.int32, (seq_count * 2 * CAP, 2 * rows), 0)
    within = slot_row % (2 * CAP)
    mixing = sum(
        jnp.where(
            (slot_row // (2 * CAP * copies) == chosen_twice[j:j + 1, :])
            & (within == wrap * CAP + slot_twice[j]),
            jnp.concatenate([gates[j], gates[j]], axis=1),
            0.0,
        )
        for j in range(TOPK)
    )
    coarse = mixing.astype(jnp.bfloat16).astype(jnp.float32)
    mix[...] = jnp.concatenate([coarse, mixing - coarse], axis=1).T.astype(jnp.bfloat16)

    mark("E3_waitw")
    for load in loads[6:9]:
        load.wait()

    def unpack(t, chunk, at):
        settle(arrived.at[t, pl.ds(0, sum(r > 0 for r in chunk))], xr.at[t, chunk_of[chunk[0]]])
        for r in chunk:
            block = arrived[t, r] if r > 0 else x_out[t, me // copies]
            stacked[t, at:at + CAP, :thin] = block[:CAP, :]
            stacked[t, at:at + CAP, thin:] = block[CAP:, :]
            at += CAP

    mark("E4_earlydots")
    far_rows = near // 2 * CAP
    for t in range(shares - 1):
        unpack(t, chunks[0], 0)
        x = stacked[t, :far_rows, :widths[t]]
        begun[0] = jnp.dot(x, rows_of(t, gate), preferred_element_type=jnp.float32)
        begun[1] = jnp.dot(x, rows_of(t, up), preferred_element_type=jnp.float32)
    final = shares - 1
    for chunk in chunks:
        mark(f"F{chunks.index(chunk)}0_recv")
        first, count = far_first.index(chunk[0]) * CAP, len(chunk) * CAP
        g = u = 0.0
        for t in range(shares):
            if t < final and first < far_rows:
                g, u = begun[0, first:first + count], begun[1, first:first + count]
                continue
            unpack(t, chunk, first)
            x = stacked[t, first:first + count, :widths[t]]
            g = g + jnp.dot(x, rows_of(t, gate), preferred_element_type=jnp.float32)
            u = u + jnp.dot(x, rows_of(t, up), preferred_element_type=jnp.float32)
        mark(f"F{chunks.index(chunk)}1_expert")
        scales = stacked[final, first:first + count, widths[-1]:widths[-1] + 2].astype(jnp.float32)
        scales = scales[:, :1] + scales[:, 1:]
        g, u = g * scales, u * scales
        hidden = (g * jax.nn.sigmoid(1.702 * g) * (u + 1.0)).astype(jnp.bfloat16)
        part = jnp.dot(hidden, down[...], preferred_element_type=jnp.float32).astype(jnp.bfloat16)
        mark(f"F{chunks.index(chunk)}2_pack")
        left, right = folded(part)
        for i, r in enumerate(chunk):
            target = back.at[r] if r > 0 else returned.at[me]
            target[:CAP] = left[i * CAP:(i + 1) * CAP, :]
            target[CAP:] = right[i * CAP:(i + 1) * CAP, :]
            if r > 0:
                returns[r].start()
    mark("G0_waitsend")
    settle(arrived.at[:, pl.ds(0, seq_count - 1)], once.at[X_SENT])
    mark("G1_waitret")
    settle(returned.at[pl.ds(0, seq_count - 1)], once.at[BACK_HERE])
    mark("G2_mix")
    parts = jnp.dot(
        mix[...], returned[...].reshape(seq_count * 2 * CAP, fold), preferred_element_type=jnp.float32
    )
    mixed = [parts[h * rows:(h + 1) * rows, :] + parts[(2 + h) * rows:(3 + h) * rows, :] for h in range(2)]
    stream = res[...].astype(jnp.float32) + out_ref[0].astype(jnp.float32)
    out_ref[1, :, :fold] = (stream[:, :fold] + mixed[0]).astype(jnp.bfloat16)
    out_ref[1, :, fold:] = (stream[:, fold:] + mixed[1][:, :D - fold]).astype(jnp.bfloat16)
    mark("G3_drain")
    settle(returned.at[pl.ds(0, seq_count - 1)], once.at[BACK_SENT])
    mark(None)


def on_device(
    residual,
    queries,
    key_rows,
    values,
    attention_sinks,
    out_weight,
    norm_gain,
    router_weight,
    gate_weight,
    up_weight,
    down_weight,
    routing,
    span_order,
):
    seq_count = lax.axis_size("seq")
    fsdp_count = lax.axis_size("fsdp")
    z_count = seq_count // 4
    rows = residual.shape[1]
    dma = pltpu.SemaphoreType.DMA
    vmem = pl.BlockSpec(memory_space=pltpu.VMEM)
    hbm = pl.BlockSpec(memory_space=pltpu.HBM)

    def held(*shape):
        return pltpu.VMEM(shape, jnp.bfloat16)

    kv_width = 2 * KVH * HD
    fold = -(-D // 256) * 128
    w_rows, columns = out_weight.shape
    shares = 2 if fsdp_count == 2 and columns % 16 == 0 else 1
    thin = -(-((columns if shares == 2 else D) + 2) // 256) * 128
    both = pl.pallas_call(
        functools.partial(layer_kernel, seq_count, fsdp_count),
        out_shape=jax.ShapeDtypeStruct((2, rows, D), jnp.bfloat16),
        in_specs=[hbm] * 13,
        out_specs=vmem,
        scratch_shapes=[
            pltpu.SMEM((1, HEADS), jnp.float32),
            pltpu.SMEM((1, span_order.shape[0]), jnp.int32),
            held(D),
            pltpu.VMEM((TOPK, rows), jnp.int32),
            held(rows, D),
            held(rows, HEADS * HD),
            held(rows, KVH * HD),
            held(rows, KVH * HD),
            held(*router_weight.shape[::-1]),
            held(*gate_weight.shape),
            held(*up_weight.shape),
            held(*down_weight.shape),
            held(seq_count, rows, kv_width),
            held(seq_count, columns, w_rows),
            held(KVH, HEADS // KVH * rows, HD),
            pltpu.VMEM((rows, seq_count * rows), jnp.float32),
            held(KVH, fsdp_count, rows, HEADS // KVH * HD),
            held(fsdp_count, rows, columns),
            held(fsdp_count, rows, columns),
            held(shares, EXPERTS, 2 * CAP, thin),
            held(shares, seq_count, 2 * CAP, thin),
            held(shares, seq_count * CAP, 2 * thin),
            pltpu.VMEM((2, seq_count // 4 * CAP, gate_weight.shape[1]), jnp.float32),
            held(seq_count, 2 * CAP, fold),
            held(seq_count, 2 * CAP, fold),
            held(4 * rows, seq_count * 2 * CAP),
            held(EXPERTS * 2 * CAP, 2 * rows),
            dma((13,)),
        ]
        + [dma((z_count,))] * 2
        + [dma((z_count + 1, 4)), dma((z_count, 4)), dma((z_count, 3)), dma((z_count,))]
        + [dma((KVH, 2, max(fsdp_count - 1, 1)))]
        + [dma((fsdp_count,))] * 2
        + [dma((shares, 3)), dma((9,))],
        compiler_params=pltpu.CompilerParams(
            collective_id=0, has_side_effects=True, vmem_limit_bytes=60 * 1024 * 1024
        ),
    )(
        attention_sinks[None, :],
        span_order[None, :],
        norm_gain,
        routing[0].T,
        residual[0],
        queries[0],
        key_rows[0],
        values[0],
        out_weight.T,
        router_weight.T,
        gate_weight,
        up_weight,
        down_weight,
    )
    return (both[0][None], both[1][None])


def solution(mesh):
    in_specs = (
        P("fsdp", "seq", None),
        P("fsdp", "seq", None),
        P("fsdp", "seq", None),
        P("fsdp", "seq", None),
        P(),
        P("seq", "fsdp"),
        P(),
        P(),
        P(None, "seq"),
        P(None, "seq"),
        P("seq", None),
        P("fsdp", "seq", None),
        P(),
    )
    out_specs = (P("fsdp", "seq", None), P("fsdp", "seq", None))
    return jax.shard_map(
        on_device, mesh=mesh, in_specs=in_specs, out_specs=out_specs, check_vma=False
    )
```
